32 devices in a mesh: seq: 8 (over y, x, core), ch: 4 (over z).
Axes of the slice: x: 2, y: 2, z: 4, core: 2. Of those that a mesh axis runs over, the one named last changes fastest.
Arguments:
- inputs: bfloat16 [256, 4096], P('ch', 'seq'), may hold values from -6 to 6
- w_value: bfloat16 [256, 256], P(None, 'ch'), may hold values from -0.375 to 0.375
- w_gate: bfloat16 [256, 256], P(None, 'ch'), may hold values from -0.375 to 0.375
- w_out: bfloat16 [256, 256], P('ch'), may hold values from -0.375 to 0.375
- filter_taps: float32 [256, 4096], P('ch', 'seq'), may hold values from -6 to 6
- grad_out: bfloat16 [256, 4096], P('ch', 'seq'), may hold values from -6 to 6
Outputs:
- d_inputs: bfloat16 [256, 4096], P('ch', 'seq')
- d_w_value: float32 [256, 256], P(None, 'ch')
- d_w_gate: float32 [256, 256], P(None, 'ch')
- d_w_out: float32 [256, 256], P('ch')
- d_filter: float32 [256, 4096], P('ch', 'seq')
The draws below stay inside these ranges and needn't reach their ends.
All inputs are finite; a program needn't handle non-finite values.
Results may differ from the reference program's by a relative error of at most 0.015.
Values may be sent and summed in bfloat16 or wider, within the bound.
A program may use at most 64 MiB of HBM per device.

```python
import math
import jax
import jax.numpy as jnp

D = 256
TOKENS = 4096


def draw_filter_taps(key, part):
    inner_key = jax.random.fold_in(key, 17)
    key_rate, key_jitter = jax.random.split(inner_key)
    upper_log = math.log(3.0 * TOKENS)
    lower_log = math.log(40.0)
    jitter = jax.random.truncated_normal(key_jitter, -6.0, 6.0, (D, TOKENS), jnp.float32)
    timescale = jnp.exp(lower_log + (upper_log - lower_log) * jax.random.uniform(key_rate, (D, 1), jnp.float32))
    decay_rate = 1.0 / timescale
    positions = jnp.arange(TOKENS, dtype=jnp.float32)[None, :]
    normalizer = jnp.sqrt((1.0 - jnp.exp(-2.0 * decay_rate)) / (1.0 - jnp.exp(-2.0 * TOKENS * decay_rate)))
    return (jitter * jnp.exp(-decay_rate * positions) * normalizer).astype(jnp.float32)


def steps_of(stream_key, shape, cuts, low, high):
    gain = 1.0
    for axis_at, parts in cuts:
        steps = jax.random.uniform(jax.random.fold_in(jax.random.fold_in(stream_key, 6), axis_at), (parts,), jnp.float32, low / len(cuts), high / len(cuts))
        gain = gain * jnp.repeat(jnp.exp(steps), shape[axis_at] // parts).reshape((-1,) + (1,) * (len(shape) - 1 - axis_at))
    return gain


def normal_values(stream_key, shape, width, bound, pieces=(), kind=jnp.bfloat16):
    result = width * jax.random.normal(stream_key, shape, jnp.float32)
    if pieces:
        result = result * steps_of(stream_key, shape, pieces, -0.22, 0.18)
    return jnp.clip(result, -bound, bound).astype(kind)


def setup_inputs(seed: int = 0) -> dict:
    seeds = jax.random.split(jax.random.key(seed), 7)
    return {
        "inputs": normal_values(seeds[0], (D, TOKENS), 1.0, 6.0, ((0, 4), (1, 8))),
        "w_value": normal_values(seeds[1], (D, D), D ** -0.5, 0.375, ((1, 4),)),
        "w_gate": normal_values(seeds[2], (D, D), D ** -0.5, 0.375, ((1, 4),)),
        "w_out": normal_values(seeds[3], (D, D), D ** -0.5, 0.375, ((0, 4),)),
        "filter_taps": draw_filter_taps(jax.random.fold_in(seeds[6], 71), 0),
        "grad_out": normal_values(seeds[5], (D, TOKENS), 1.0, 6.0, ((0, 4), (1, 8))),
    }


def reference(inputs, w_value, w_gate, w_out, filter_taps, grad_out):
    padded_len = 2 * TOKENS
    value_proj = jnp.dot(w_value.T, inputs, preferred_element_type=jnp.float32)
    gate_proj = jnp.dot(w_gate.T, inputs, preferred_element_type=jnp.float32)
    spec_filter = jnp.fft.rfft(filter_taps, n=padded_len, axis=1)
    spec_value = jnp.fft.rfft(value_proj, n=padded_len, axis=1)
    mixed_seq = jnp.fft.irfft(spec_filter * spec_value, n=padded_len, axis=1)[:, :TOKENS]
    gated_out = (gate_proj * mixed_seq).astype(jnp.bfloat16)
    d_gated = jnp.dot(w_out, grad_out, preferred_element_type=jnp.float32)
    d_gate = (d_gated * mixed_seq).astype(jnp.bfloat16)
    d_mixed = d_gated * gate_proj
    spec_grad = jnp.fft.rfft(d_mixed, n=padded_len, axis=1)
    d_value = jnp.fft.irfft(jnp.conj(spec_filter) * spec_grad, n=padded_len, axis=1)[:, :TOKENS]
    d_value = d_value.astype(jnp.bfloat16)
    filter_raw = jnp.fft.irfft(jnp.conj(spec_value) * spec_grad, n=padded_len, axis=1)[:, :TOKENS]
    grad_scale = TOKENS ** -0.5
    d_inputs = jnp.dot(w_value, d_value, preferred_element_type=jnp.float32)
    d_inputs = d_inputs + jnp.dot(w_gate, d_gate, preferred_element_type=jnp.float32)
    d_inputs = d_inputs.astype(jnp.bfloat16)
    d_w_value = jnp.dot(inputs, d_value.T, preferred_element_type=jnp.float32) * grad_scale
    d_w_gate = jnp.dot(inputs, d_gate.T, preferred_element_type=jnp.float32) * grad_scale
    d_w_out = jnp.dot(gated_out, grad_out.T, preferred_element_type=jnp.float32) * grad_scale
    d_filter = filter_raw.astype(jnp.float32) * grad_scale
    return d_inputs, d_w_value, d_w_gate, d_w_out, d_filter
```

```python
import functools
import math

import jax
import jax.numpy as jnp
import numpy as np
from jax import lax
from jax.experimental import pallas as pl
from jax.experimental.pallas import tpu as pltpu
from jax.sharding import PartitionSpec as P

F32 = jnp.float32
BF16 = jnp.bfloat16
LANES = 128


def dft_tables(strides, lanes, chans):
    length = 2 * strides * lanes
    n1 = np.arange(strides)
    n2 = np.arange(lanes)
    half = np.arange(strides) + 0.5
    first = np.exp(-2j * np.pi * np.outer(half, n1) / (2 * strides))
    eye = np.eye(chans)
    first_re, first_im = np.kron(first.real, eye), np.kron(first.imag, eye)
    ahead = np.concatenate([first_re, first_im], 0)
    twist = np.repeat(np.exp(-2j * np.pi * np.outer(half, n2) / length), chans, axis=0)
    last = np.exp(-2j * np.pi * np.outer(n2, n2) / lanes)
    c, s = last.real, last.imag
    across = np.block([[c, s], [-s, c]])
    low = lambda a: jnp.asarray(a.astype(np.float32)).astype(BF16)
    wide = lambda a: jnp.asarray(a.astype(np.float32))
    return (
        low(ahead),
        low(ahead.T * (2.0 / length)),
        low(across),
        low(across.T),
        wide(np.stack([twist.real, twist.imag])),
    )


def each(count, step):
    if count <= 16:
        for k in range(count):
            step(k)
    else:
        lax.fori_loop(0, count, lambda k, carry: (step(k), carry)[1], 0)


def near(count):
    if count & (count - 1):
        return None
    return [1 << b for b in range(count.bit_length() - 1)]


def body(
    groups, rings,
    in_hbm, wv_hbm, wg_hbm, wo_hbm, filt_hbm, grad_hbm, ahead_hbm, back_hbm, across_hbm, return_hbm, twist_hbm,
    din_ref, dw_ref, dfil_ref,
    full_in, full_grad, got_filt, out_val, got_val, out_dif, got_dif,
    out_mix, got_mix, out_dv, got_dv, out_df, got_df,
    out_din, got_din, out_w, got_w, out_ws, got_ws, out_v, got_v, out_vs, got_vs,
    wv_ref, wg_ref, wo_ref, filt_ref, ahead_ref, back_ref, across_ref, return_ref, twist_ref,
    seq_send, seq_recv, ch_send, ch_recv, line_send, line_recv, table_sem, fetch_sem, round_sem,
):
    me = lax.axis_index("seq")
    mc = lax.axis_index("ch")
    ch_rows, tokens = in_hbm.shape
    chans = ch_rows // groups
    tiles = tokens // LANES
    width = full_in.shape[0] * ch_rows
    barrier = pltpu.get_barrier_semaphore()

    def seq_peer(k):
        return lax.rem(me + k, groups)

    def ch_peer(k):
        return lax.rem(mc + k, rings)

    hops = near(groups)

    def can(step):
        return mc < rings - 1 if step == 1 else mc > 0

    def greet(semaphore):
        for hop_by in hops:
            pl.semaphore_signal(
                semaphore, inc=1, device_id={"seq": me ^ hop_by}, device_id_type=pl.DeviceIdType.MESH)

    greet(barrier)
    for step in (1, -1):
        @pl.when(can(step))
        def _():
            pl.semaphore_signal(
                barrier, inc=1, device_id={"ch": mc + step}, device_id_type=pl.DeviceIdType.MESH)
    tables = [
        pltpu.make_async_copy(src, dst, table_sem.at[i])
        for i, (src, dst) in enumerate((
            (ahead_hbm, ahead_ref), (twist_hbm, twist_ref), (across_hbm, across_ref),
            (return_hbm, return_ref), (back_hbm, back_ref),
            (wv_hbm, wv_ref), (wg_hbm, wg_ref), (wo_hbm, wo_ref)))
    ]
    fetches = [
        pltpu.make_async_copy(src, dst, fetch_sem.at[i])
        for i, (src, dst) in enumerate((
            (in_hbm, full_in.at[mc]), (grad_hbm, full_grad.at[mc]), (filt_hbm, filt_ref)))
    ]
    for copy in fetches + tables:
        copy.start()
    between = (mc > 0) & (mc < rings - 1)

    @pl.when(between)
    def _():
        pl.semaphore_wait(barrier, len(hops) + 2)

    @pl.when(jnp.logical_not(between))
    def _():
        pl.semaphore_wait(barrier, len(hops) + 1)


    def seq_copy(stage, src, dst, k, pick):
        return pltpu.make_async_remote_copy(
            src_ref=src.at[seq_peer(k)] if pick else src,
            dst_ref=dst.at[me],
            send_sem=seq_send.at[stage],
            recv_sem=seq_recv.at[stage],
            device_id={"seq": seq_peer(k)},
            device_id_type=pl.DeviceIdType.MESH,
        )

    def ch_copy(src, dst, k):
        return pltpu.make_async_remote_copy(
            src_ref=src.at[ch_peer(k)],
            dst_ref=dst.at[mc],
            send_sem=ch_send.at[0],
            recv_sem=ch_recv.at[0],
            device_id={"ch": ch_peer(k)},
            device_id_type=pl.DeviceIdType.MESH,
        )

    def seq_start(stage, src, dst, pick=True):
        each(groups - 1, lambda k: seq_copy(stage, src, dst, k + 1, pick).start())

    def took(ref, count, semaphore):
        blocks = ref.at[pl.ds(0, count)]
        pltpu.make_async_copy(blocks, blocks, semaphore).wait()

    def seq_wait(stage, src, dst, pick=True):
        took(dst, groups - 1, seq_recv.at[stage])

    def seq_done(stage, src, dst, pick=True):
        took(dst, groups - 1, seq_send.at[stage])

    wholes = (full_in, full_grad)

    def hop(array, block, step):
        return pltpu.make_async_remote_copy(
            src_ref=wholes[array].at[block],
            dst_ref=wholes[array].at[block],
            send_sem=line_send.at[array, (step + 1) // 2, block],
            recv_sem=line_recv.at[array, block],
            device_id={"ch": mc + step},
            device_id_type=pl.DeviceIdType.MESH,
        )

    def present(step, far):
        return mc >= far if step == 1 else mc < rings - far

    def line_open(array):
        for step in (1, -1):
            @pl.when(can(step))
            def _():
                hop(array, mc, step).start()

    def line_take(array, far):
        for step in (1, -1):
            @pl.when(present(step, far))
            def _():
                hop(array, mc - step * far, step).wait_recv()
                if far < rings - 1:
                    @pl.when(can(step))
                    def _():
                        hop(array, mc - step * far, step).start()

    def line_close(array):
        for step in (1, -1):
            @pl.when(can(step))
            def _():
                hop(array, mc, step).wait_send()
                for far in range(1, rings - 1):
                    @pl.when(present(step, far))
                    def _():
                        hop(array, mc - step * far, step).wait_send()

    fetches[0].wait()
    line_open(0)
    fetches[1].wait()
    line_open(1)
    for turn in range(len(hops) - 1):
        greet(round_sem.at[turn])
        pl.semaphore_wait(round_sem.at[turn], len(hops))
    fetches[2].wait()
    seq_start(0, filt_ref, got_filt)
    got_filt[me] = filt_ref[me]

    def by_owner(x):
        x = x.reshape(groups, chans, tokens)
        return jnp.concatenate([x[:, :, j * LANES:(j + 1) * LANES] for j in range(tiles)], axis=1)

    def by_token(x):
        x = x.astype(F32)
        x = jnp.concatenate([x[:, j * chans:(j + 1) * chans, :] for j in range(tiles)], axis=2)
        return x.reshape(ch_rows, tokens)

    def stacked(ref):
        return jnp.concatenate([ref[p] for p in range(groups)], axis=0).astype(BF16)

    rows = ahead_ref.shape[1]

    def dot(a, b):
        return jnp.dot(a, b, preferred_element_type=F32)

    def spectrum(x):
        first = dot(ahead_ref[...], x)
        re, im = first[:rows], first[rows:]
        tw_re, tw_im = twist_ref[0], twist_ref[1]
        mid = jnp.concatenate([re * tw_re - im * tw_im, re * tw_im + im * tw_re], axis=1).astype(BF16)
        out = dot(mid, across_ref[...])
        return out[:, :LANES], out[:, LANES:]

    def signal(re, im):
        mid = dot(jnp.concatenate([re, im], axis=1).astype(BF16), return_ref[...])
        re, im = mid[:, :LANES], mid[:, LANES:]
        tw_re, tw_im = twist_ref[0], twist_ref[1]
        tall = jnp.concatenate([re * tw_re + im * tw_im, im * tw_re - re * tw_im], axis=0).astype(BF16)
        return dot(back_ref[...], tall).reshape(groups, tiles * chans, LANES)

    over_first = (((0,), (0,)), ((), ()))
    over_last = (((1,), (1,)), ((), ()))
    for far in range(1, rings - 1):
        line_take(0, far)
        line_take(1, far)

    for table in tables:
        table.wait()
    seq_wait(0, filt_ref, got_filt)
    by_tile = jnp.concatenate(
        [got_filt[p][:, j * LANES:(j + 1) * LANES] for p in range(groups) for j in range(tiles)], axis=0)
    f_re, f_im = spectrum(by_tile.astype(BF16))

    line_take(0, rings - 1)
    x_in = full_in[...].reshape(width, tokens)
    value = dot(wv_ref[...], x_in)
    out_val[...] = by_owner(value).astype(BF16)
    seq_start(1, out_val, got_val)
    got_val[me] = out_val[me]
    gate = dot(wg_ref[...], x_in)

    line_take(1, rings - 1)
    x_grad = full_grad[...].reshape(width, tokens)
    d_gated = dot(wo_ref[...], x_grad)
    out_dif[...] = by_owner(d_gated * gate).astype(BF16)
    seq_start(2, out_dif, got_dif)
    got_dif[me] = out_dif[me]

    seq_wait(1, out_val, got_val)
    v_re, v_im = spectrum(stacked(got_val))
    out_mix[...] = signal(f_re * v_re - f_im * v_im, f_re * v_im + f_im * v_re).astype(BF16)
    seq_start(3, out_mix, got_mix)
    got_mix[me] = out_mix[me]

    seq_wait(2, out_dif, got_dif)
    g_re, g_im = spectrum(stacked(got_dif))
    out_dv[...] = signal(f_re * g_re + f_im * g_im, f_re * g_im - f_im * g_re).astype(BF16)
    seq_start(4, out_dv, got_dv)
    got_dv[me] = out_dv[me]
    out_df[...] = signal(v_re * g_re + v_im * g_im, v_re * g_im - v_im * g_re).astype(BF16)
    seq_start(5, out_df, got_df)
    got_df[me] = out_df[me]

    parts = width // LANES

    def by_share(x):
        x = x.reshape(groups, chans, width)
        return jnp.concatenate([x[:, :, j * LANES:(j + 1) * LANES] for j in range(parts)], axis=1)

    def by_width(x):
        return jnp.concatenate([x[:, j * chans:(j + 1) * chans, :] for j in range(parts)], axis=2).reshape(ch_rows, width)

    def total(ref):
        out = ref[0].astype(F32)
        for p in range(1, ref.shape[0]):
            out = out + ref[p].astype(F32)
        return out.astype(BF16)

    seq_wait(3, out_mix, got_mix)
    mixed = by_token(got_mix[...])
    gated_out = (gate * mixed).astype(BF16)
    d_gate = (d_gated * mixed).astype(BF16)
    gate_term = lax.dot_general(d_gate, x_in, over_last, preferred_element_type=F32)
    out_term = lax.dot_general(gated_out, x_grad, over_last, preferred_element_type=F32)
    out_w[...] = jnp.concatenate([by_share(gate_term), by_share(out_term)], axis=1).astype(BF16)
    seq_start(6, out_w, got_w)
    got_w[me] = out_w[me]
    from_gate = lax.dot_general(wg_ref[...], d_gate, over_first, preferred_element_type=F32)

    seq_wait(4, out_dv, got_dv)
    d_value = by_token(got_dv[...]).astype(BF16)
    value_term = lax.dot_general(d_value, x_in, over_last, preferred_element_type=F32)
    out_v[...] = by_share(value_term).astype(BF16)
    seq_start(8, out_v, got_v)
    d_in = lax.dot_general(wv_ref[...], d_value, over_first, preferred_element_type=F32) + from_gate
    out_din[...] = d_in.reshape(rings, ch_rows, tokens).astype(BF16)
    each(rings - 1, lambda k: ch_copy(out_din, got_din, k + 1).start())
    got_v[me] = out_v[me]
    got_din[mc] = out_din[mc]

    seq_wait(6, out_w, got_w)
    out_ws[...] = total(got_w)
    seq_start(7, out_ws, got_ws, False)
    got_ws[me] = out_ws[...]

    seq_wait(5, out_df, got_df)
    dfil_ref[...] = by_token(got_df[...]).astype(BF16)

    seq_wait(8, out_v, got_v)
    out_vs[...] = total(got_v)
    seq_start(9, out_vs, got_vs, False)
    got_vs[me] = out_vs[...]

    seq_wait(7, out_ws, got_ws, False)
    half = parts * chans
    summed = got_ws[...].astype(F32)
    dw_ref[1] = by_width(summed[:, :half, :]).astype(BF16)
    dw_ref[2] = by_width(summed[:, half:, :]).astype(BF16)
    took(got_din, rings - 1, ch_recv.at[0])
    din_ref[...] = total(got_din)
    seq_wait(9, out_vs, got_vs, False)
    dw_ref[0] = by_width(got_vs[...].astype(F32)).astype(BF16)

    line_close(0)
    line_close(1)
    took(got_din, rings - 1, ch_send.at[0])
    for stage, src, dst, pick in (
        (0, filt_ref, got_filt, True), (1, out_val, got_val, True), (2, out_dif, got_dif, True),
        (3, out_mix, got_mix, True), (4, out_dv, got_dv, True), (5, out_df, got_df, True),
        (6, out_w, got_w, True), (7, out_ws, got_ws, False), (8, out_v, got_v, True), (9, out_vs, got_vs, False),
    ):
        seq_done(stage, src, dst, pick)


def finish(scale, din_ref, dw_ref, dfil_ref, din_out, dwv_out, dwg_out, dwo_out, dfil_out):
    din_out[...] = din_ref[...]
    dwv_out[...] = dw_ref[0].astype(F32) * scale
    dwg_out[...] = dw_ref[1].astype(F32) * scale
    dwo_out[...] = dw_ref[2].astype(F32) * scale
    dfil_out[...] = dfil_ref[...].astype(F32) * scale


def solution(mesh):
    groups, rings = mesh.shape["seq"], mesh.shape["ch"]

    def on_device(inputs, w_value, w_gate, w_out, filter_taps, grad_out):
        ch_rows, tokens = inputs.shape
        width = w_value.shape[0]
        chans, tiles, parts = ch_rows // groups, tokens // LANES, width // LANES
        tables = dft_tables(groups * tiles, LANES, chans)
        scale = 1.0 / math.sqrt(tokens * groups)
        vmem = pl.BlockSpec(memory_space=pltpu.VMEM)
        hbm = pl.BlockSpec(memory_space=pltpu.HBM)
        block = pltpu.VMEM((groups, tiles * chans, LANES), BF16)
        whole = pltpu.VMEM((rings, ch_rows, tokens), BF16)
        share = lambda count: [
            pltpu.VMEM((groups, count * parts * chans, LANES), BF16),
            pltpu.VMEM((groups, count * parts * chans, LANES), BF16),
            pltpu.VMEM((count * parts * chans, LANES), BF16),
            pltpu.VMEM((groups, count * parts * chans, LANES), BF16),
        ]
        tokens_out = jax.ShapeDtypeStruct((ch_rows, tokens), F32)
        weight_out = jax.ShapeDtypeStruct((ch_rows, width), F32)
        d_inputs, d_weights, d_filter = pl.pallas_call(
            functools.partial(body, groups, rings),
            out_shape=(
                pltpu.VMEM((ch_rows, tokens), BF16),
                pltpu.VMEM((3, ch_rows, width), BF16),
                pltpu.VMEM((ch_rows, tokens), BF16),
            ),
            in_specs=[hbm] * 11,
            out_specs=(vmem,) * 3,
            scratch_shapes=[whole, whole, pltpu.VMEM((groups, chans, tokens), F32)] + [block] * 10
            + [whole, whole] + share(2) + share(1)
            + [pltpu.VMEM((ch_rows, width), BF16)] * 3 + [pltpu.VMEM((groups, chans, tokens), F32)]
            + [pltpu.VMEM(table.shape, table.dtype) for table in tables] + [
                pltpu.SemaphoreType.DMA((10,)),
                pltpu.SemaphoreType.DMA((10,)),
                pltpu.SemaphoreType.DMA((1,)),
                pltpu.SemaphoreType.DMA((1,)),
                pltpu.SemaphoreType.DMA((2, 2, rings)),
                pltpu.SemaphoreType.DMA((2, rings)),
                pltpu.SemaphoreType.DMA((8,)),
                pltpu.SemaphoreType.DMA((3,)),
                pltpu.SemaphoreType.REGULAR((max(len(near(groups)) - 1, 1),)),
            ],
            compiler_params=pltpu.CompilerParams(collective_id=0, has_side_effects=True),
        )(
            inputs, w_value.T, w_gate.T, w_out, filter_taps.reshape(groups, chans, tokens), grad_out, *tables,
        )
        d_inputs, d_w_value, d_w_gate, d_w_out, d_filter = pl.pallas_call(
            functools.partial(finish, scale),
            out_shape=(
                jax.ShapeDtypeStruct((ch_rows, tokens), BF16), weight_out, weight_out, weight_out, tokens_out,
            ),
            in_specs=[vmem] * 3,
            out_specs=(vmem,) * 5,
            compiler_params=pltpu.CompilerParams(vmem_limit_bytes=8 << 20),
        )(d_inputs, d_weights, d_filter)
        return d_inputs, d_w_value.T, d_w_gate.T, d_w_out, d_filter

    return jax.shard_map(
        on_device,
        mesh=mesh,
        in_specs=(P("ch", "seq"), P(None, "ch"), P(None, "ch"), P("ch", None), P("ch", "seq"), P("ch", "seq")),
        out_specs=(P("ch", "seq"), P(None, "ch"), P(None, "ch"), P("ch", None), P("ch", "seq")),
        check_vma=False,
    )
```

```python
import functools
import math

import jax
import jax.numpy as jnp
import numpy as np
from jax import lax
from jax.experimental import pallas as pl
from jax.experimental.pallas import tpu as pltpu
from jax.sharding import PartitionSpec as P

F32 = jnp.float32
BF16 = jnp.bfloat16
LANES = 128


def dft_tables(strides, lanes, chans):
    length = 2 * strides * lanes
    n1 = np.arange(strides)
    n2 = np.arange(lanes)
    half = np.arange(strides) + 0.5
    first = np.exp(-2j * np.pi * np.outer(half, n1) / (2 * strides))
    eye = np.eye(chans)
    first_re, first_im = np.kron(first.real, eye), np.kron(first.imag, eye)
    ahead = np.concatenate([first_re, first_im], 0)
    twist = np.repeat(np.exp(-2j * np.pi * np.outer(half, n2) / length), chans, axis=0)
    last = np.exp(-2j * np.pi * np.outer(n2, n2) / lanes)
    c, s = last.real, last.imag
    across = np.block([[c, s], [-s, c]])
    low = lambda a: jnp.asarray(a.astype(np.float32)).astype(BF16)
    wide = lambda a: jnp.asarray(a.astype(np.float32))
    return (
        low(ahead),
        low(ahead.T * (2.0 / length)),
        low(across),
        low(across.T),
        wide(np.stack([twist.real, twist.imag])),
    )


def each(count, step):
    if count <= 16:
        for k in range(count):
            step(k)
    else:
        lax.fori_loop(0, count, lambda k, carry: (step(k), carry)[1], 0)


def near(count):
    return [1 << b for b in range(count.bit_length() - 1)]


def body(
    groups, rings,
    in_hbm, wv_hbm, wg_hbm, wo_hbm, filt_hbm, grad_hbm, ahead_hbm, back_hbm, across_hbm, return_hbm, twist_hbm,
    din_ref, dw_ref, dfil_ref,
    full_in, full_grad, filt_ref, weights, out_filt, got_filt, out_val, got_val, out_dif, got_dif,
    out_mix, got_mix, out_dv, got_dv, out_df, got_df,
    out_din, got_din, out_w, got_w, out_ws, got_ws, out_v, got_v, out_vs, got_vs,
    ahead_ref, back_ref, across_ref, return_ref, twist_ref,
    seq_send, seq_recv, din_send, din_recv, line_send, line_recv, weight_send, weight_recv,
    table_sem, fetch_sem, round_sem,
):
    me = lax.axis_index("seq")
    mc = lax.axis_index("ch")
    ch_rows, tokens = in_hbm.shape
    chans = ch_rows // groups
    tiles = tokens // LANES
    width = full_in.shape[0] * ch_rows
    parts = width // LANES
    half = rings // 2
    right = lax.div(mc, half)
    toward = 1 - 2 * right
    worker = half - 1 + right
    other = half - right
    slot = (worker - mc) * toward
    works = slot == 0
    rests = slot > 0
    between = (mc > 0) & (mc < rings - 1)
    barrier = pltpu.get_barrier_semaphore()
    hops = near(groups)

    def can(step):
        return mc < rings - 1 if step == 1 else mc > 0

    def greet(semaphore):
        for step in (1, -1):
            @pl.when(can(step))
            def _():
                pl.semaphore_signal(
                    semaphore, inc=1, device_id={"ch": mc + step}, device_id_type=pl.DeviceIdType.MESH)
        for hop_by in hops:
            pl.semaphore_signal(
                semaphore, inc=1, device_id={"seq": me ^ hop_by}, device_id_type=pl.DeviceIdType.MESH)

    def greeted(semaphore):
        @pl.when(between)
        def _():
            pl.semaphore_wait(semaphore, len(hops) + 2)

        @pl.when(jnp.logical_not(between))
        def _():
            pl.semaphore_wait(semaphore, len(hops) + 1)

    greet(barrier)
    fetches = [
        pltpu.make_async_copy(src, dst, fetch_sem.at[i])
        for i, (src, dst) in enumerate((
            (in_hbm, full_in.at[mc]), (grad_hbm, full_grad.at[mc]),
            (wv_hbm, weights.at[0, 0]), (wg_hbm, weights.at[0, 1]), (wo_hbm, weights.at[0, 2]),
            (filt_hbm, filt_ref)))
    ]
    tables = [
        pltpu.make_async_copy(src, dst, table_sem.at[i])
        for i, (src, dst) in enumerate((
            (ahead_hbm, ahead_ref), (twist_hbm, twist_ref), (across_hbm, across_ref),
            (return_hbm, return_ref), (back_hbm, back_ref)))
    ]
    for copy in fetches:
        copy.start()

    @pl.when(works)
    def _():
        for copy in tables:
            copy.start()

    greeted(barrier)

    def send(src, dst, sems, seq, ch):
        return pltpu.make_async_remote_copy(
            src_ref=src, dst_ref=dst, send_sem=sems[0], recv_sem=sems[1],
            device_id={"seq": seq, "ch": ch}, device_id_type=pl.DeviceIdType.MESH)

    def stage_sems(stage):
        return seq_send.at[stage], seq_recv.at[stage]

    def seq_peer(k):
        return lax.rem(me + k, groups)

    def took(ref, count, semaphore):
        blocks = ref.at[pl.ds(0, count)]
        pltpu.make_async_copy(blocks, blocks, semaphore).wait()

    def scatter(stage, src, dst, ch, skip, base=0):
        each(groups - skip, lambda k: send(
            src.at[base + seq_peer(k + skip)], dst, stage_sems(stage), seq_peer(k + skip), ch).start())

    def spread(stage, src, dst):
        each(groups - 1, lambda k: send(
            src, dst.at[me], stage_sems(stage), seq_peer(k + 1), mc).start())

    def to_planes(stage, src, dst):
        for s in range(half):
            scatter(stage, src, dst.at[me], mc - toward * s, 1 if s == 0 else 0, s * groups)
        dst[me] = src[me]

    wholes = (full_in, full_grad)

    def hop(array, block, k):
        return send(
            wholes[array].at[block], wholes[array].at[block],
            (line_send.at[array, k], line_recv.at[array, block]), me, mc + toward)

    def pass_on(array):
        for k in range(1, half):
            @pl.when(slot < half - k)
            def _():
                hop(array, mc - toward * k, k).wait_recv()
                hop(array, mc - toward * k, k).start()

    def take_inner(array):
        for k in range(half):
            hop(array, other + toward * k, 0).wait_recv()

    def weight_copy(kind, s):
        return send(weights.at[0, kind], weights.at[s, kind], (weight_send.at[kind], weight_recv.at[s, kind]), me, worker)

    for array in range(2):
        fetches[array].wait()
        hop(array, mc, 0).start()
    for kind in range(3):
        fetches[2 + kind].wait()

        @pl.when(rests)
        def _():
            weight_copy(kind, slot).start()

    for turn in range(len(hops) + half - 2):
        greet(round_sem.at[turn])
        greeted(round_sem.at[turn])

    def by_owner(x):
        x = x.reshape(groups, chans, tokens)
        return jnp.concatenate([x[:, :, j * LANES:(j + 1) * LANES] for j in range(tiles)], axis=1).astype(BF16)

    def by_token(x):
        x = x.astype(F32)
        x = jnp.concatenate([x[:, j * chans:(j + 1) * chans, :] for j in range(tiles)], axis=2)
        return x.reshape(ch_rows, tokens)

    fetches[5].wait()
    out_filt[...] = by_owner(filt_ref[...])

    @pl.when(rests)
    def _():
        scatter(0, out_filt, got_filt.at[slot * groups + me], worker, 0)

    @pl.when(works)
    def _():
        scatter(0, out_filt, got_filt.at[me], mc, 1)
        got_filt[me] = out_filt[me]

    for array in range(2):
        pass_on(array)

    def by_share(x):
        x = x.reshape(groups, chans, width)
        return jnp.concatenate([x[:, :, j * LANES:(j + 1) * LANES] for j in range(parts)], axis=1)

    def by_width(x):
        return jnp.concatenate([x[:, j * chans:(j + 1) * chans, :] for j in range(parts)], axis=2).reshape(ch_rows, width)

    def total(ref):
        out = ref[0].astype(F32)
        for p in range(1, ref.shape[0]):
            out = out + ref[p].astype(F32)
        return out.astype(BF16)

    rows = ahead_ref.shape[1]

    def dot(a, b):
        return jnp.dot(a, b, preferred_element_type=F32)

    def lanes(x, s):
        return x[:, s * LANES:(s + 1) * LANES]

    def spectrum(xs):
        first = dot(ahead_ref[...], jnp.concatenate(xs, axis=1))
        tw_re, tw_im = twist_ref[0], twist_ref[1]
        mids = []
        for s in range(half):
            re, im = lanes(first[:rows], s), lanes(first[rows:], s)
            mids.append(jnp.concatenate([re * tw_re - im * tw_im, re * tw_im + im * tw_re], axis=1).astype(BF16))
        out = dot(jnp.concatenate(mids, axis=0), across_ref[...])
        return out[:, :LANES], out[:, LANES:]

    def signal(re, im):
        mid = dot(jnp.concatenate([re, im], axis=1).astype(BF16), return_ref[...])
        tw_re, tw_im = twist_ref[0], twist_ref[1]
        talls = []
        for s in range(half):
            part = mid[s * rows:(s + 1) * rows]
            re, im = part[:, :LANES], part[:, LANES:]
            talls.append(jnp.concatenate([re * tw_re + im * tw_im, im * tw_re - re * tw_im], axis=0).astype(BF16))
        out = dot(back_ref[...], jnp.concatenate(talls, axis=1))
        return [lanes(out, s).reshape(groups, tiles * chans, LANES).astype(BF16) for s in range(half)]

    def slots(x):
        size = x.shape[0] // half
        return [x[s * size:(s + 1) * size] for s in range(half)]

    def stacked(ref):
        return [jnp.concatenate([ref[p, s] for p in range(groups)], axis=0) for s in range(half)]

    def put(ref, xs):
        for s in range(half):
            ref[:, s] = xs[s]

    def put_flat(ref, xs):
        for s in range(half):
            ref[s * groups:(s + 1) * groups] = xs[s]

    def exchange(stage, src, dst):
        scatter(stage, src, dst.at[me], mc, 1)
        dst[me] = src[me]

    def tokens_of(ref):
        return jnp.concatenate([by_token(ref[:, s]) for s in range(half)], axis=0)

    def weight(kind):
        return jnp.concatenate([weights[s, kind] for s in range(half)], axis=0)

    over_first = (((0,), (0,)), ((), ()))
    over_last = (((1,), (1,)), ((), ()))

    @pl.when(works)
    def _():
        take_inner(0)
        for s in range(1, half):
            for kind in range(3):
                weight_copy(kind, s).wait_recv()
        x_in = full_in[...].reshape(width, tokens)
        w_value = weight(0)
        w_gate = weight(1)
        put(out_val, [by_owner(x) for x in slots(dot(w_value, x_in))])
        exchange(1, out_val, got_val)
        gate = dot(w_gate, x_in)

        take_inner(1)
        x_grad = full_grad[...].reshape(width, tokens)
        d_gated = dot(weight(2), x_grad)
        put(out_dif, [by_owner(x) for x in slots(d_gated * gate)])
        exchange(2, out_dif, got_dif)

        for table in tables:
            table.wait()
        took(got_val, groups - 1, seq_recv.at[1])
        v_re, v_im = spectrum(stacked(got_val))
        took(got_filt, half * groups - 1, seq_recv.at[0])
        f_re, f_im = spectrum([
            jnp.concatenate([got_filt[s * groups + p] for p in range(groups)], axis=0) for s in range(half)])
        put(out_mix, signal(f_re * v_re - f_im * v_im, f_re * v_im + f_im * v_re))
        exchange(3, out_mix, got_mix)

        took(got_dif, groups - 1, seq_recv.at[2])
        g_re, g_im = spectrum(stacked(got_dif))
        put(out_dv, signal(f_re * g_re + f_im * g_im, f_re * g_im - f_im * g_re))
        exchange(4, out_dv, got_dv)
        put_flat(out_df, signal(v_re * g_re + v_im * g_im, v_re * g_im - v_im * g_re))
        to_planes(5, out_df, got_df)

        took(got_mix, groups - 1, seq_recv.at[3])
        mixed = tokens_of(got_mix)
        gated_out = (gate * mixed).astype(BF16)
        d_gate = (d_gated * mixed).astype(BF16)
        gate_term = lax.dot_general(d_gate, x_in, over_last, preferred_element_type=F32)
        out_term = lax.dot_general(gated_out, x_grad, over_last, preferred_element_type=F32)
        put_flat(out_w, [
            jnp.concatenate([by_share(a), by_share(b)], axis=1).astype(BF16)
            for a, b in zip(slots(gate_term), slots(out_term))])
        to_planes(6, out_w, got_w)
        from_gate = lax.dot_general(w_gate, d_gate, over_first, preferred_element_type=F32)

        took(got_dv, groups - 1, seq_recv.at[4])
        d_value = tokens_of(got_dv).astype(BF16)
        value_term = lax.dot_general(d_value, x_in, over_last, preferred_element_type=F32)
        put_flat(out_v, [by_share(a).astype(BF16) for a in slots(value_term)])
        to_planes(8, out_v, got_v)
        d_in = lax.dot_general(w_value, d_value, over_first, preferred_element_type=F32) + from_gate
        out_din[...] = d_in.reshape(rings, ch_rows, tokens).astype(BF16)
        outward = [mc - toward * s for s in range(1, half)]
        for block in outward + [other + toward * k for k in reversed(range(half))]:
            send(out_din.at[block], got_din.at[right], (din_send.at[0], din_recv.at[0]), me, block).start()
        got_din[right] = out_din[mc]

    def when_count(semaphore, ref, working, resting):
        @pl.when(works)
        def _():
            took(ref, working, semaphore)

        @pl.when(rests)
        def _():
            took(ref, resting, semaphore)

    when_count(seq_recv.at[6], got_w, groups - 1, groups)
    out_ws[...] = total(got_w)
    spread(7, out_ws, got_ws)
    got_ws[me] = out_ws[...]

    when_count(seq_recv.at[5], got_df, groups - 1, groups)
    dfil_ref[...] = by_token(got_df[...]).astype(BF16)

    when_count(seq_recv.at[8], got_v, groups - 1, groups)
    out_vs[...] = total(got_v)
    spread(9, out_vs, got_vs)
    got_vs[me] = out_vs[...]

    took(got_ws, groups - 1, seq_recv.at[7])
    size = parts * chans
    summed = got_ws[...].astype(F32)
    dw_ref[1] = by_width(summed[:, :size, :]).astype(BF16)
    dw_ref[2] = by_width(summed[:, size:, :]).astype(BF16)
    when_count(din_recv.at[0], got_din, 1, 2)
    din_ref[...] = total(got_din)
    took(got_vs, groups - 1, seq_recv.at[9])
    dw_ref[0] = by_width(got_vs[...].astype(F32)).astype(BF16)

    for array in range(2):
        hop(array, mc, 0).wait_send()
        for k in range(1, half):
            @pl.when(slot < half - k)
            def _():
                hop(array, mc - toward * k, k).wait_send()

    @pl.when(works)
    def _():
        took(out_filt, groups - 1, seq_send.at[0])
        for stage, src in ((1, out_val), (2, out_dif), (3, out_mix), (4, out_dv)):
            took(src, groups - 1, seq_send.at[stage])
        for stage, src in ((5, out_df), (6, out_w), (8, out_v)):
            took(src, half * groups - 1, seq_send.at[stage])
        took(out_din, rings - 1, din_send.at[0])

    @pl.when(rests)
    def _():
        took(out_filt, groups, seq_send.at[0])
        for kind in range(3):
            weight_copy(kind, slot).wait_send()

    took(got_ws, groups - 1, seq_send.at[7])
    took(got_vs, groups - 1, seq_send.at[9])


def finish(scale, din_ref, dw_ref, dfil_ref, din_out, dwv_out, dwg_out, dwo_out, dfil_out):
    din_out[...] = din_ref[...]
    dwv_out[...] = dw_ref[0].astype(F32) * scale
    dwg_out[...] = dw_ref[1].astype(F32) * scale
    dwo_out[...] = dw_ref[2].astype(F32) * scale
    dfil_out[...] = dfil_ref[...].astype(F32) * scale


def solution(mesh):
    groups, rings = mesh.shape["seq"], mesh.shape["ch"]

    def on_device(inputs, w_value, w_gate, w_out, filter_taps, grad_out):
        ch_rows, tokens = inputs.shape
        width = w_value.shape[0]
        chans, tiles, parts = ch_rows // groups, tokens // LANES, width // LANES
        tables = dft_tables(groups * tiles, LANES, chans)
        scale = 1.0 / math.sqrt(tokens * groups)
        vmem = pl.BlockSpec(memory_space=pltpu.VMEM)
        hbm = pl.BlockSpec(memory_space=pltpu.HBM)
        half = rings // 2
        block = pltpu.VMEM((groups, half, tiles * chans, LANES), BF16)
        flat = pltpu.VMEM((half * groups, tiles * chans, LANES), BF16)
        plane = pltpu.VMEM((groups, tiles * chans, LANES), BF16)
        whole = pltpu.VMEM((rings, ch_rows, tokens), BF16)
        share = lambda count: [
            pltpu.VMEM((half * groups, count * parts * chans, LANES), BF16),
            pltpu.VMEM((groups, count * parts * chans, LANES), BF16),
            pltpu.VMEM((count * parts * chans, LANES), BF16),
            pltpu.VMEM((groups, count * parts * chans, LANES), BF16),
        ]
        tokens_out = jax.ShapeDtypeStruct((ch_rows, tokens), F32)
        weight_out = jax.ShapeDtypeStruct((ch_rows, width), F32)
        d_inputs, d_weights, d_filter = pl.pallas_call(
            functools.partial(body, groups, rings),
            out_shape=(
                pltpu.VMEM((ch_rows, tokens), BF16),
                pltpu.VMEM((3, ch_rows, width), BF16),
                pltpu.VMEM((ch_rows, tokens), BF16),
            ),
            in_specs=[hbm] * 11,
            out_specs=(vmem,) * 3,
            scratch_shapes=[
                whole, whole, pltpu.VMEM((ch_rows, tokens), F32), pltpu.VMEM((half, 3, ch_rows, width), BF16),
                plane, flat] + [block] * 8 + [flat, plane]
            + [whole, pltpu.VMEM((2, ch_rows, tokens), BF16)] + share(2) + share(1)
            + [pltpu.VMEM(table.shape, table.dtype) for table in tables] + [
                pltpu.SemaphoreType.DMA((10,)),
                pltpu.SemaphoreType.DMA((10,)),
                pltpu.SemaphoreType.DMA((1,)),
                pltpu.SemaphoreType.DMA((1,)),
                pltpu.SemaphoreType.DMA((2, half)),
                pltpu.SemaphoreType.DMA((2, rings)),
                pltpu.SemaphoreType.DMA((3,)),
                pltpu.SemaphoreType.DMA((half, 3)),
                pltpu.SemaphoreType.DMA((5,)),
                pltpu.SemaphoreType.DMA((6,)),
                pltpu.SemaphoreType.REGULAR((len(near(groups)) + half - 2,)),
            ],
            compiler_params=pltpu.CompilerParams(collective_id=0, has_side_effects=True),
        )(
            inputs, w_value.T, w_gate.T, w_out, filter_taps, grad_out, *tables,
        )
        d_inputs, d_w_value, d_w_gate, d_w_out, d_filter = pl.pallas_call(
            functools.partial(finish, scale),
            out_shape=(
                jax.ShapeDtypeStruct((ch_rows, tokens), BF16), weight_out, weight_out, weight_out, tokens_out,
            ),
            in_specs=[vmem] * 3,
            out_specs=(vmem,) * 5,
            compiler_params=pltpu.CompilerParams(vmem_limit_bytes=8 << 20),
        )(d_inputs, d_weights, d_filter)
        return d_inputs, d_w_value.T, d_w_gate.T, d_w_out, d_filter

    return jax.shard_map(
        on_device,
        mesh=mesh,
        in_specs=(P("ch", "seq"), P(None, "ch"), P(None, "ch"), P("ch", None), P("ch", "seq"), P("ch", "seq")),
        out_specs=(P("ch", "seq"), P(None, "ch"), P(None, "ch"), P("ch", None), P("ch", "seq")),
        check_vma=False,
    )
```

```python
import functools
import math

import jax
import jax.numpy as jnp
import numpy as np
from jax import lax
from jax.experimental import pallas as pl
from jax.experimental.pallas import tpu as pltpu
from jax.sharding import PartitionSpec as P

F32 = jnp.float32
BF16 = jnp.bfloat16
LANES = 128


def dft_tables(strides, lanes, chans):
    length = 2 * strides * lanes
    n1 = np.arange(strides)
    n2 = np.arange(lanes)
    half = np.arange(strides) + 0.5
    first = np.exp(-2j * np.pi * np.outer(half, n1) / (2 * strides))
    eye = np.eye(chans)
    first_re, first_im = np.kron(first.real, eye), np.kron(first.imag, eye)
    ahead = np.concatenate([first_re, first_im], 0)
    twist = np.repeat(np.exp(-2j * np.pi * np.outer(half, n2) / length), chans, axis=0)
    last = np.exp(-2j * np.pi * np.outer(n2, n2) / lanes)
    c, s = last.real, last.imag
    across = np.block([[c, s], [-s, c]])
    low = lambda a: jnp.asarray(a.astype(np.float32)).astype(BF16)
    wide = lambda a: jnp.asarray(a.astype(np.float32))
    return (
        low(ahead),
        low(ahead.T * (2.0 / length)),
        low(across),
        low(across.T),
        wide(np.stack([twist.real, twist.imag])),
    )


def each(count, step):
    if count <= 16:
        for k in range(count):
            step(k)
    else:
        lax.fori_loop(0, count, lambda k, carry: (step(k), carry)[1], 0)


def near(count):
    return [1 << b for b in range(count.bit_length() - 1)]


def body(
    groups, rings,
    in_hbm, wv_hbm, wg_hbm, wo_hbm, filt_hbm, grad_hbm, ahead_hbm, back_hbm, across_hbm, return_hbm, twist_hbm,
    din_ref, dw_ref, dfil_ref,
    full_in, full_grad, filt_ref, weights, out_filt, got_filt, out_val, got_val, out_dif, got_dif,
    out_mix, got_mix, out_dv, got_dv, out_df, got_df,
    out_din, got_din, out_w, got_w, out_ws, got_ws, out_v, got_v,
    ahead_ref, back_ref, across_ref, return_ref, twist_ref,
    seq_send, seq_recv, din_send, din_recv, line_send, line_recv, share_send, share_recv,
    table_sem, fetch_sem, round_sem,
):
    me = lax.axis_index("seq")
    mc = lax.axis_index("ch")
    ch_rows, tokens = in_hbm.shape
    chans = ch_rows // groups
    tiles = tokens // LANES
    width = full_in.shape[0] * ch_rows
    parts = width // LANES
    half = rings // 2
    splits = weights.shape[1]
    right = lax.div(mc, half)
    toward = 1 - 2 * right
    worker = half - 1 + right
    other = half - right
    slot = (worker - mc) * toward
    works = slot == 0
    rests = slot > 0
    between = (mc > 0) & (mc < rings - 1)
    barrier = pltpu.get_barrier_semaphore()
    hops = near(groups)

    def can(step):
        return mc < rings - 1 if step == 1 else mc > 0

    def greet(semaphore):
        for step in (1, -1):
            @pl.when(can(step))
            def _():
                pl.semaphore_signal(
                    semaphore, inc=1, device_id={"ch": mc + step}, device_id_type=pl.DeviceIdType.MESH)
        for hop_by in hops:
            pl.semaphore_signal(
                semaphore, inc=1, device_id={"seq": me ^ hop_by}, device_id_type=pl.DeviceIdType.MESH)

    def greeted(semaphore):
        @pl.when(between)
        def _():
            pl.semaphore_wait(semaphore, len(hops) + 2)

        @pl.when(jnp.logical_not(between))
        def _():
            pl.semaphore_wait(semaphore, len(hops) + 1)

    greet(barrier)
    fetches = [
        pltpu.make_async_copy(src, dst, fetch_sem.at[i])
        for i, (src, dst) in enumerate((
            (in_hbm, full_in.at[mc]), (grad_hbm, full_grad.at[mc]),
            (wv_hbm, weights.at[0, :, 0]), (wg_hbm, weights.at[0, :, 1]), (wo_hbm, weights.at[0, :, 2]),
            (filt_hbm, filt_ref)))
    ]
    tables = [
        pltpu.make_async_copy(src, dst, table_sem.at[i])
        for i, (src, dst) in enumerate((
            (ahead_hbm, ahead_ref), (twist_hbm, twist_ref), (across_hbm, across_ref),
            (return_hbm, return_ref), (back_hbm, back_ref)))
    ]
    for copy in fetches:
        copy.start()

    @pl.when(works)
    def _():
        for copy in tables:
            copy.start()

    greeted(barrier)

    def send(src, dst, sems, seq, ch):
        return pltpu.make_async_remote_copy(
            src_ref=src, dst_ref=dst, send_sem=sems[0], recv_sem=sems[1],
            device_id={"seq": seq, "ch": ch}, device_id_type=pl.DeviceIdType.MESH)

    def stage_sems(stage):
        return seq_send.at[stage], seq_recv.at[stage]

    def seq_peer(k):
        return lax.rem(me + k, groups)

    def took(ref, count, semaphore):
        blocks = ref.at[pl.ds(0, count)]
        pltpu.make_async_copy(blocks, blocks, semaphore).wait()

    def scatter(stage, src, dst, ch, skip, base=0):
        each(groups - skip, lambda k: send(
            src.at[base + seq_peer(k + skip)], dst, stage_sems(stage), seq_peer(k + skip), ch).start())

    def spread(stage, src, dst):
        each(groups - 1, lambda k: send(
            src, dst.at[me], stage_sems(stage), seq_peer(k + 1), mc).start())

    def to_planes(stage, src, dst):
        for s in range(half):
            scatter(stage, src, dst.at[me], mc - toward * s, 1 if s == 0 else 0, s * groups)
        dst[me] = src[me]

    def to_owners(stage, src, dst):
        for s in range(1, half):
            each(groups, lambda k: send(
                src.at[seq_peer(k), s], dst.at[me, 0], stage_sems(stage), seq_peer(k), mc - toward * s).start())

    wholes = (full_in, full_grad)

    def block_to(array, block, ch, k):
        return send(
            wholes[array].at[block], wholes[array].at[block],
            (line_send.at[array, k], line_recv.at[array, block]), me, ch)

    def take(array):
        for k in range(1, rings):
            block_to(array, lax.rem(mc + k, rings), mc, 0).wait_recv()

    def pass_on(array):
        for s in range(1, half):
            inner = [mc - toward * t for t in range(1, half) if t != s]
            for block in [other + toward * k for k in range(half)] + inner:
                block_to(array, block, mc - toward * s, 1).start()

    mine = lax.rem(me, splits)

    def share_up(s):
        return send(weights.at[0, mine], weights.at[s, mine], (share_send.at[0], share_recv.at[s, 0]), me, worker)

    def share_across(s, k):
        return send(
            weights.at[s, mine], weights.at[s, mine], (share_send.at[s], share_recv.at[s, 1]), me ^ k, mc)

    for kind in range(3):
        fetches[2 + kind].wait()

    @pl.when(rests)
    def _():
        share_up(slot).start()

    for array in range(2):
        fetches[array].wait()

        @pl.when(works)
        def _():
            block_to(array, mc, other, 0).start()

        @pl.when(rests)
        def _():
            block_to(array, mc, worker, 1).start()

    for turn in range(len(hops) + half - 2):
        greet(round_sem.at[turn])
        greeted(round_sem.at[turn])
        if turn == half - 2:
            for array in range(2):
                @pl.when(works)
                def _():
                    for s in range(1, half):
                        block_to(array, mc, mc - toward * s, 1).start()

                @pl.when(rests)
                def _():
                    block_to(array, mc, other, 0).start()

    def by_owner(x):
        x = x.reshape(groups, chans, tokens)
        return jnp.concatenate([x[:, :, j * LANES:(j + 1) * LANES] for j in range(tiles)], axis=1).astype(BF16)

    def by_token(x):
        x = x.astype(F32)
        x = jnp.concatenate([x[:, j * chans:(j + 1) * chans, :] for j in range(tiles)], axis=2)
        return x.reshape(ch_rows, tokens)

    fetches[5].wait()
    out_filt[...] = by_owner(filt_ref[...])

    @pl.when(rests)
    def _():
        scatter(0, out_filt, got_filt.at[slot * groups + me], worker, 0)

    @pl.when(works)
    def _():
        scatter(0, out_filt, got_filt.at[me], mc, 1)
        got_filt[me] = out_filt[me]

    @pl.when(works)
    def _():
        for s in range(1, half):
            share_up(s).wait_recv()
            for k in range(1, splits):
                share_across(s, k).start()

    def by_share(x):
        x = x.reshape(groups, chans, width)
        return jnp.concatenate([x[:, :, j * LANES:(j + 1) * LANES] for j in range(parts)], axis=1)

    def by_width(x):
        return jnp.concatenate([x[:, j * chans:(j + 1) * chans, :] for j in range(parts)], axis=2).reshape(ch_rows, width)

    def total(ref):
        out = ref[0].astype(F32)
        for p in range(1, ref.shape[0]):
            out = out + ref[p].astype(F32)
        return out.astype(BF16)

    rows = ahead_ref.shape[1]

    def dot(a, b):
        return jnp.dot(a, b, preferred_element_type=F32)

    def lanes(x, s):
        return x[:, s * LANES:(s + 1) * LANES]

    def spectrum(xs):
        first = dot(ahead_ref[...], jnp.concatenate(xs, axis=1))
        tw_re, tw_im = twist_ref[0], twist_ref[1]
        mids = []
        for s in range(half):
            re, im = lanes(first[:rows], s), lanes(first[rows:], s)
            mids.append(jnp.concatenate([re * tw_re - im * tw_im, re * tw_im + im * tw_re], axis=1).astype(BF16))
        out = dot(jnp.concatenate(mids, axis=0), across_ref[...])
        return out[:, :LANES], out[:, LANES:]

    def signal(re, im):
        mid = dot(jnp.concatenate([re, im], axis=1).astype(BF16), return_ref[...])
        tw_re, tw_im = twist_ref[0], twist_ref[1]
        talls = []
        for s in range(half):
            part = mid[s * rows:(s + 1) * rows]
            re, im = part[:, :LANES], part[:, LANES:]
            talls.append(jnp.concatenate([re * tw_re + im * tw_im, im * tw_re - re * tw_im], axis=0).astype(BF16))
        out = dot(back_ref[...], jnp.concatenate(talls, axis=1))
        return [lanes(out, s).reshape(groups, tiles * chans, LANES).astype(BF16) for s in range(half)]

    def slots(x):
        size = x.shape[0] // half
        return [x[s * size:(s + 1) * size] for s in range(half)]

    def stacked(ref):
        return [jnp.concatenate([ref[p, s] for p in range(groups)], axis=0) for s in range(half)]

    def put(ref, xs):
        for s in range(half):
            ref[:, s] = xs[s]

    def put_flat(ref, xs):
        for s in range(half):
            ref[s * groups:(s + 1) * groups] = xs[s]

    def exchange(stage, src, dst):
        scatter(stage, src, dst.at[me], mc, 1)
        dst[me] = src[me]

    def tokens_of(ref, count):
        return jnp.concatenate([by_token(ref[:, s]) for s in range(count)], axis=0)

    def weight(kind, count):
        return jnp.concatenate([weights[s, q, kind] for s in range(count) for q in range(splits)], axis=0)

    def reduce_weights(gate, d_gated, d_gate, mixed, x_in, x_grad):
        gated_out = (gate[:ch_rows] * mixed[:ch_rows]).astype(BF16)
        gate_term = lax.dot_general(d_gate[:ch_rows], x_in, over_last, preferred_element_type=F32)
        out_term = lax.dot_general(gated_out, x_grad, over_last, preferred_element_type=F32)
        out_w[...] = jnp.concatenate([by_share(gate_term), by_share(out_term)], axis=1).astype(BF16)
        exchange(6, out_w, got_w)

    def reduce_value(d_value, x_in):
        value_term = lax.dot_general(d_value[:ch_rows], x_in, over_last, preferred_element_type=F32)
        out_v[...] = value_term.astype(BF16)
        spread(8, out_v, got_v)

    over_first = (((0,), (0,)), ((), ()))
    over_last = (((1,), (1,)), ((), ()))

    @pl.when(works)
    def _():
        take(0)
        for s in range(1, half):
            across = weights.at[s, pl.ds(0, splits - 1)]
            pltpu.make_async_copy(across, across, share_recv.at[s, 1]).wait()
        x_in = full_in[...].reshape(width, tokens)
        w_value = weight(0, half)
        w_gate = weight(1, half)
        put(out_val, [by_owner(x) for x in slots(dot(w_value, x_in))])
        exchange(1, out_val, got_val)
        pass_on(0)
        gate = dot(w_gate, x_in)

        take(1)
        x_grad = full_grad[...].reshape(width, tokens)
        d_gated = dot(weight(2, half), x_grad)
        put(out_dif, [by_owner(x) for x in slots(d_gated * gate)])
        exchange(2, out_dif, got_dif)
        pass_on(1)

        for table in tables:
            table.wait()
        took(got_val, groups - 1, seq_recv.at[1])
        v_re, v_im = spectrum(stacked(got_val))
        took(got_filt, half * groups - 1, seq_recv.at[0])
        f_re, f_im = spectrum([
            jnp.concatenate([got_filt[s * groups + p] for p in range(groups)], axis=0) for s in range(half)])
        put(out_mix, signal(f_re * v_re - f_im * v_im, f_re * v_im + f_im * v_re))
        to_owners(10, out_mix, got_mix)
        exchange(3, out_mix, got_mix)

        took(got_dif, groups - 1, seq_recv.at[2])
        g_re, g_im = spectrum(stacked(got_dif))
        put(out_dv, signal(f_re * g_re + f_im * g_im, f_re * g_im - f_im * g_re))
        to_owners(11, out_dv, got_dv)
        exchange(4, out_dv, got_dv)
        put_flat(out_df, signal(v_re * g_re + v_im * g_im, v_re * g_im - v_im * g_re))
        to_planes(5, out_df, got_df)

        took(got_mix, groups - 1, seq_recv.at[3])
        mixed = tokens_of(got_mix, half)
        d_gate = (d_gated * mixed).astype(BF16)
        reduce_weights(gate, d_gated, d_gate, mixed, x_in, x_grad)
        from_gate = lax.dot_general(w_gate, d_gate, over_first, preferred_element_type=F32)

        took(got_dv, groups - 1, seq_recv.at[4])
        d_value = tokens_of(got_dv, half).astype(BF16)
        reduce_value(d_value, x_in)
        d_in = lax.dot_general(w_value, d_value, over_first, preferred_element_type=F32) + from_gate
        out_din[...] = d_in.reshape(rings, ch_rows, tokens).astype(BF16)
        outward = [mc - toward * s for s in range(1, half)]
        for block in outward + [other + toward * k for k in reversed(range(half))]:
            send(out_din.at[block], got_din.at[right], (din_send.at[0], din_recv.at[0]), me, block).start()
        got_din[right] = out_din[mc]

    @pl.when(rests)
    def _():
        take(0)
        x_in = full_in[...].reshape(width, tokens)
        gate = dot(weight(1, 1), x_in)
        take(1)
        x_grad = full_grad[...].reshape(width, tokens)
        d_gated = dot(weight(2, 1), x_grad)
        took(got_mix, groups // half, seq_recv.at[10])
        mixed = tokens_of(got_mix, 1)
        d_gate = (d_gated * mixed).astype(BF16)
        reduce_weights(gate, d_gated, d_gate, mixed, x_in, x_grad)
        took(got_dv, groups // half, seq_recv.at[11])
        reduce_value(tokens_of(got_dv, 1).astype(BF16), x_in)

    def when_count(semaphore, ref, working, resting):
        @pl.when(works)
        def _():
            took(ref, working, semaphore)

        @pl.when(rests)
        def _():
            took(ref, resting, semaphore)

    took(got_w, groups - 1, seq_recv.at[6])
    out_ws[...] = total(got_w)
    spread(7, out_ws, got_ws)
    got_ws[me] = out_ws[...]
    got_v[me] = out_v[...]

    when_count(seq_recv.at[5], got_df, groups - 1, groups)
    dfil_ref[...] = by_token(got_df[...]).astype(BF16)

    took(got_v, groups - 1, seq_recv.at[8])
    dw_ref[0] = total(got_v)
    when_count(din_recv.at[0], got_din, 1, 2)
    din_ref[...] = total(got_din)
    took(got_ws, groups - 1, seq_recv.at[7])
    size = parts * chans
    summed = got_ws[...].astype(F32)
    dw_ref[1] = by_width(summed[:, :size, :]).astype(BF16)
    dw_ref[2] = by_width(summed[:, size:, :]).astype(BF16)

    for array in range(2):
        block_to(array, mc, other, 0).wait_send()

        @pl.when(works)
        def _():
            for s in range(1, half):
                took(wholes[array], rings - 1, line_send.at[array, 1])

        @pl.when(rests)
        def _():
            block_to(array, mc, worker, 1).wait_send()

    @pl.when(works)
    def _():
        took(out_filt, groups - 1, seq_send.at[0])
        for stage, src in ((1, out_val), (2, out_dif), (3, out_mix), (4, out_dv)):
            took(src, groups - 1, seq_send.at[stage])
        for stage, src in ((10, out_mix), (11, out_dv)):
            took(src, (half - 1) * groups // half, seq_send.at[stage])
        took(out_df, half * groups - 1, seq_send.at[5])
        took(out_din, rings - 1, din_send.at[0])
        for s in range(1, half):
            took(weights.at[s], splits - 1, share_send.at[s])

    @pl.when(rests)
    def _():
        took(out_filt, groups, seq_send.at[0])
        share_up(slot).wait_send()

    for stage, src in ((6, got_w), (7, got_ws), (8, got_v)):
        took(src, groups - 1, seq_send.at[stage])


def finish(scale, din_ref, dw_ref, dfil_ref, din_out, dwv_out, dwg_out, dwo_out, dfil_out):
    din_out[...] = din_ref[...]
    dwv_out[...] = dw_ref[0].astype(F32) * scale
    dwg_out[...] = dw_ref[1].astype(F32) * scale
    dwo_out[...] = dw_ref[2].astype(F32) * scale
    dfil_out[...] = dfil_ref[...].astype(F32) * scale


def solution(mesh):
    groups, rings = mesh.shape["seq"], mesh.shape["ch"]

    def on_device(inputs, w_value, w_gate, w_out, filter_taps, grad_out):
        ch_rows, tokens = inputs.shape
        width = w_value.shape[0]
        chans, tiles, parts = ch_rows // groups, tokens // LANES, width // LANES
        tables = dft_tables(groups * tiles, LANES, chans)
        scale = 1.0 / math.sqrt(tokens * groups)
        vmem = pl.BlockSpec(memory_space=pltpu.VMEM)
        hbm = pl.BlockSpec(memory_space=pltpu.HBM)
        half = rings // 2
        block = pltpu.VMEM((groups, half, tiles * chans, LANES), BF16)
        flat = pltpu.VMEM((half * groups, tiles * chans, LANES), BF16)
        plane = pltpu.VMEM((groups, tiles * chans, LANES), BF16)
        whole = pltpu.VMEM((rings, ch_rows, tokens), BF16)
        splits = min(groups, ch_rows // 16)
        split = lambda w: w.reshape(splits, ch_rows // splits, width)
        share = pltpu.VMEM((groups, 2 * parts * chans, LANES), BF16)
        rows_of = pltpu.VMEM((ch_rows, width), BF16)
        tokens_out = jax.ShapeDtypeStruct((ch_rows, tokens), F32)
        weight_out = jax.ShapeDtypeStruct((ch_rows, width), F32)
        d_inputs, d_weights, d_filter = pl.pallas_call(
            functools.partial(body, groups, rings),
            out_shape=(
                pltpu.VMEM((ch_rows, tokens), BF16),
                pltpu.VMEM((3, ch_rows, width), BF16),
                pltpu.VMEM((ch_rows, tokens), BF16),
            ),
            in_specs=[hbm] * 11,
            out_specs=(vmem,) * 3,
            scratch_shapes=[
                whole, whole, pltpu.VMEM((ch_rows, tokens), F32), pltpu.VMEM((half, splits, 3, ch_rows // splits, width), BF16),
                plane, flat] + [block] * 8 + [flat, plane]
            + [whole, pltpu.VMEM((2, ch_rows, tokens), BF16)]
            + [share, share, pltpu.VMEM((2 * parts * chans, LANES), BF16), share, rows_of, pltpu.VMEM((groups, ch_rows, width), BF16)]
            + [pltpu.VMEM(table.shape, table.dtype) for table in tables] + [
                pltpu.SemaphoreType.DMA((12,)),
                pltpu.SemaphoreType.DMA((12,)),
                pltpu.SemaphoreType.DMA((1,)),
                pltpu.SemaphoreType.DMA((1,)),
                pltpu.SemaphoreType.DMA((2, 2)),
                pltpu.SemaphoreType.DMA((2, rings)),
                pltpu.SemaphoreType.DMA((half,)),
                pltpu.SemaphoreType.DMA((half, 2)),
                pltpu.SemaphoreType.DMA((5,)),
                pltpu.SemaphoreType.DMA((6,)),
                pltpu.SemaphoreType.REGULAR((len(near(groups)) + half - 2,)),
            ],
            compiler_params=pltpu.CompilerParams(collective_id=0, has_side_effects=True),
        )(
            inputs, split(w_value.T), split(w_gate.T), split(w_out), filter_taps, grad_out, *tables,
        )
        d_inputs, d_w_value, d_w_gate, d_w_out, d_filter = pl.pallas_call(
            functools.partial(finish, scale),
            out_shape=(
                jax.ShapeDtypeStruct((ch_rows, tokens), BF16), weight_out, weight_out, weight_out, tokens_out,
            ),
            in_specs=[vmem] * 3,
            out_specs=(vmem,) * 5,
            compiler_params=pltpu.CompilerParams(vmem_limit_bytes=8 << 20),
        )(d_inputs, d_weights, d_filter)
        return d_inputs, d_w_value.T, d_w_gate.T, d_w_out, d_filter

    return jax.shard_map(
        on_device,
        mesh=mesh,
        in_specs=(P("ch", "seq"), P(None, "ch"), P(None, "ch"), P("ch", None), P("ch", "seq"), P("ch", "seq")),
        out_specs=(P("ch", "seq"), P(None, "ch"), P(None, "ch"), P("ch", None), P("ch", "seq")),
        check_vma=False,
    )
```

```python
import functools
import math

import jax
import jax.numpy as jnp
import numpy as np
from jax import lax
from jax.experimental import pallas as pl
from jax.experimental.pallas import tpu as pltpu
from jax.sharding import PartitionSpec as P

F32 = jnp.float32
BF16 = jnp.bfloat16
LANES = 128


def dft_tables(strides, lanes, chans):
    length = 2 * strides * lanes
    n1 = np.arange(strides)
    n2 = np.arange(lanes)
    half = np.arange(strides) + 0.5
    first = np.exp(-2j * np.pi * np.outer(half, n1) / (2 * strides))
    eye = np.eye(chans)
    first_re, first_im = np.kron(first.real, eye), np.kron(first.imag, eye)
    ahead = np.concatenate([first_re, first_im], 0)
    twist = np.repeat(np.exp(-2j * np.pi * np.outer(half, n2) / length), chans, axis=0)
    last = np.exp(-2j * np.pi * np.outer(n2, n2) / lanes)
    c, s = last.real, last.imag
    across = np.block([[c, s], [-s, c]])
    low = lambda a: jnp.asarray(a.astype(np.float32)).astype(BF16)
    wide = lambda a: jnp.asarray(a.astype(np.float32))
    return (
        low(ahead),
        low(ahead.T * (2.0 / length)),
        low(across),
        low(across.T),
        wide(np.stack([twist.real, twist.imag])),
    )


def each(count, step):
    if count <= 16:
        for k in range(count):
            step(k)
    else:
        lax.fori_loop(0, count, lambda k, carry: (step(k), carry)[1], 0)


def near(count):
    return [1 << b for b in range(count.bit_length() - 1)]


def body(
    groups, rings,
    in_hbm, wv_hbm, wg_hbm, wo_hbm, filt_hbm, grad_hbm, ahead_hbm, back_hbm, across_hbm, return_hbm, twist_hbm,
    din_ref, dw_ref, dfil_ref,
    full_in, full_grad, filt_ref, weights, out_filt, got_filt, out_val, got_val, out_dif, got_dif,
    out_mix, got_mix, out_dv, got_dv, out_df, got_df,
    out_din, got_din, out_w, got_w, out_ws, got_ws, out_v, got_v, gate_ref, gated_ref,
    ahead_ref, back_ref, across_ref, return_ref, twist_ref,
    seq_send, seq_recv, din_send, din_recv, line_send, line_recv, share_send, share_recv,
    table_sem, fetch_sem, round_sem,
):
    me = lax.axis_index("seq")
    mc = lax.axis_index("ch")
    ch_rows, tokens = in_hbm.shape
    chans = ch_rows // groups
    tiles = tokens // LANES
    width = full_in.shape[0] * ch_rows
    parts = width // LANES
    half = rings // 2
    splits = weights.shape[1]
    right = lax.div(mc, half)
    toward = 1 - 2 * right
    worker = half - 1 + right
    other = half - right
    slot = (worker - mc) * toward
    works = slot == 0
    rests = slot > 0
    between = (mc > 0) & (mc < rings - 1)
    barrier = pltpu.get_barrier_semaphore()
    hops = near(groups)

    def can(step):
        return mc < rings - 1 if step == 1 else mc > 0

    def greet(semaphore):
        for step in (1, -1):
            @pl.when(can(step))
            def _():
                pl.semaphore_signal(
                    semaphore, inc=1, device_id={"ch": mc + step}, device_id_type=pl.DeviceIdType.MESH)
        for hop_by in hops:
            pl.semaphore_signal(
                semaphore, inc=1, device_id={"seq": me ^ hop_by}, device_id_type=pl.DeviceIdType.MESH)

    def greeted(semaphore):
        @pl.when(between)
        def _():
            pl.semaphore_wait(semaphore, len(hops) + 2)

        @pl.when(jnp.logical_not(between))
        def _():
            pl.semaphore_wait(semaphore, len(hops) + 1)

    greet(barrier)
    fetches = [
        pltpu.make_async_copy(src, dst, fetch_sem.at[i])
        for i, (src, dst) in enumerate((
            (in_hbm, full_in.at[mc]), (grad_hbm, full_grad.at[mc]),
            (wv_hbm, weights.at[0, :, 0]), (wg_hbm, weights.at[0, :, 1]), (wo_hbm, weights.at[0, :, 2]),
            (filt_hbm, filt_ref)))
    ]
    tables = [
        pltpu.make_async_copy(src, dst, table_sem.at[i])
        for i, (src, dst) in enumerate((
            (ahead_hbm, ahead_ref), (twist_hbm, twist_ref), (across_hbm, across_ref),
            (return_hbm, return_ref), (back_hbm, back_ref)))
    ]
    for copy in fetches:
        copy.start()

    for copy in tables:
        copy.start()

    greeted(barrier)

    def send(src, dst, sems, seq, ch):
        return pltpu.make_async_remote_copy(
            src_ref=src, dst_ref=dst, send_sem=sems[0], recv_sem=sems[1],
            device_id={"seq": seq, "ch": ch}, device_id_type=pl.DeviceIdType.MESH)

    def stage_sems(stage):
        return seq_send.at[stage], seq_recv.at[stage]

    def seq_peer(k):
        return lax.rem(me + k, groups)

    def took(ref, count, semaphore):
        blocks = ref.at[pl.ds(0, count)]
        pltpu.make_async_copy(blocks, blocks, semaphore).wait()

    def scatter(stage, src, dst, ch, skip, base=0):
        each(groups - skip, lambda k: send(
            src.at[base + seq_peer(k + skip)], dst, stage_sems(stage), seq_peer(k + skip), ch).start())

    def spread(stage, src, dst):
        each(groups - 1, lambda k: send(
            src, dst.at[me], stage_sems(stage), seq_peer(k + 1), mc).start())

    def to_planes(stage, src, dst):
        for s in range(half):
            scatter(stage, src, dst.at[me], mc - toward * s, 1 if s == 0 else 0, s * groups)
        dst[me] = src[me]

    wholes = (full_in, full_grad)

    def block_to(array, block, ch, k):
        return send(
            wholes[array].at[block], wholes[array].at[block],
            (line_send.at[array, k], line_recv.at[array, block]), me, ch)

    def take(array, blocks):
        for block in blocks:
            block_to(array, block, mc, 0).wait_recv()

    def pass_on(array, block):
        for s in range(1, half):
            block_to(array, block, mc - toward * s, 1).start()

    def pass_inner(array):
        for s in range(1, half):
            for t in range(1, half):
                if t != s:
                    block_to(array, mc - toward * t, mc - toward * s, 1).start()

    far_blocks = [other + toward * k for k in range(1, half)]
    outer_blocks = [mc - toward * k for k in range(1, half)]

    mine = lax.rem(me, splits)

    def share_up(s):
        return send(weights.at[0, mine], weights.at[s, mine], (share_send.at[0], share_recv.at[s, 0]), me, worker)

    def share_across(s, k):
        return send(
            weights.at[s, mine], weights.at[s, mine], (share_send.at[s], share_recv.at[s, 1]), me ^ k, mc)

    for kind in range(3):
        fetches[2 + kind].wait()

    @pl.when(rests)
    def _():
        share_up(slot).start()

    for array in range(2):
        fetches[array].wait()

        @pl.when(works)
        def _():
            block_to(array, mc, other, 0).start()

        @pl.when(rests)
        def _():
            block_to(array, mc, worker, 1).start()

    for turn in range(len(hops) + half - 2):
        greet(round_sem.at[turn])
        greeted(round_sem.at[turn])
        if turn == half - 2:
            for array in range(2):
                @pl.when(works)
                def _():
                    for s in range(1, half):
                        block_to(array, mc, mc - toward * s, 1).start()

                @pl.when(rests)
                def _():
                    block_to(array, mc, other, 0).start()

    def by_owner(x):
        x = x.reshape(groups, chans, tokens)
        return jnp.concatenate([x[:, :, j * LANES:(j + 1) * LANES] for j in range(tiles)], axis=1).astype(BF16)

    def by_token(x):
        x = x.astype(F32)
        x = jnp.concatenate([x[:, j * chans:(j + 1) * chans, :] for j in range(tiles)], axis=2)
        return x.reshape(ch_rows, tokens)

    fetches[5].wait()
    out_filt[...] = by_owner(filt_ref[...])

    scatter(0, out_filt, got_filt.at[me], mc, 1)
    got_filt[me] = out_filt[me]

    @pl.when(works)
    def _():
        for s in range(1, half):
            share_up(s).wait_recv()
            for k in range(1, splits):
                share_across(s, k).start()

    def by_share(x):
        x = x.reshape(groups, chans, width)
        return jnp.concatenate([x[:, :, j * LANES:(j + 1) * LANES] for j in range(parts)], axis=1)

    def by_width(x):
        return jnp.concatenate([x[:, j * chans:(j + 1) * chans, :] for j in range(parts)], axis=2).reshape(ch_rows, width)

    def total(ref):
        out = ref[0].astype(F32)
        for p in range(1, ref.shape[0]):
            out = out + ref[p].astype(F32)
        return out.astype(BF16)

    rows = ahead_ref.shape[1]

    def dot(a, b):
        return jnp.dot(a, b, preferred_element_type=F32)

    def spectrum(x):
        first = dot(ahead_ref[...], x)
        re, im = first[:rows], first[rows:]
        tw_re, tw_im = twist_ref[0], twist_ref[1]
        mid = jnp.concatenate([re * tw_re - im * tw_im, re * tw_im + im * tw_re], axis=1).astype(BF16)
        out = dot(mid, across_ref[...])
        return out[:, :LANES], out[:, LANES:]

    def signal(re, im):
        mid = dot(jnp.concatenate([re, im], axis=1).astype(BF16), return_ref[...])
        re, im = mid[:, :LANES], mid[:, LANES:]
        tw_re, tw_im = twist_ref[0], twist_ref[1]
        tall = jnp.concatenate([re * tw_re + im * tw_im, im * tw_re - re * tw_im], axis=0).astype(BF16)
        return dot(back_ref[...], tall).reshape(groups, tiles * chans, LANES).astype(BF16)

    def slots(x):
        size = x.shape[0] // half
        return [x[s * size:(s + 1) * size] for s in range(half)]

    def stacked(ref):
        return jnp.concatenate([ref[p] for p in range(groups)], axis=0)

    def put_flat(ref, xs):
        for s in range(half):
            ref[s * groups:(s + 1) * groups] = xs[s]

    def exchange(stage, src, dst):
        scatter(stage, src, dst.at[me], mc, 1)
        dst[me] = src[me]

    def weight(kind, count):
        return jnp.concatenate([weights[s, q, kind] for s in range(count) for q in range(splits)], axis=0)

    def reduce_weights(gate, d_gated, d_gate, mixed, x_in, x_grad):
        gated_out = (gate[:ch_rows] * mixed[:ch_rows]).astype(BF16)
        gate_term = lax.dot_general(d_gate[:ch_rows], x_in, over_last, preferred_element_type=F32)
        out_term = lax.dot_general(gated_out, x_grad, over_last, preferred_element_type=F32)
        out_w[...] = jnp.concatenate([by_share(gate_term), by_share(out_term)], axis=1).astype(BF16)
        exchange(6, out_w, got_w)

    def reduce_value(d_value, x_in):
        value_term = lax.dot_general(d_value[:ch_rows], x_in, over_last, preferred_element_type=F32)
        out_v[...] = value_term.astype(BF16)
        spread(8, out_v, got_v)

    over_first = (((0,), (0,)), ((), ()))
    over_last = (((1,), (1,)), ((), ()))

    def when_count(semaphore, ref, working, resting):
        @pl.when(works)
        def _():
            took(ref, working, semaphore)

        @pl.when(rests)
        def _():
            took(ref, resting, semaphore)

    @pl.when(works)
    def _():
        for array in range(2):
            take(array, [other])
            pass_on(array, other)
        take(0, outer_blocks + far_blocks)
        for s in range(1, half):
            across = weights.at[s, pl.ds(0, splits - 1)]
            pltpu.make_async_copy(across, across, share_recv.at[s, 1]).wait()
        x_in = full_in[...].reshape(width, tokens)
        put_flat(out_val, [by_owner(x) for x in slots(dot(weight(0, half), x_in))])
        to_planes(1, out_val, got_val)
        gate = dot(weight(1, half), x_in)
        gate_ref[...] = gate[:ch_rows]
        take(1, outer_blocks + far_blocks)
        x_grad = full_grad[...].reshape(width, tokens)
        d_gated = dot(weight(2, half), x_grad)
        put_flat(out_dif, [by_owner(x) for x in slots(d_gated * gate)])
        to_planes(2, out_dif, got_dif)
        gated_ref[...] = d_gated[:ch_rows]
        for array in range(2):
            for block in far_blocks:
                pass_on(array, block)
            pass_inner(array)

    for table in tables:
        table.wait()
    took(got_filt, groups - 1, seq_recv.at[0])
    f_re, f_im = spectrum(stacked(got_filt))
    when_count(seq_recv.at[1], got_val, groups - 1, groups)
    v_re, v_im = spectrum(stacked(got_val))
    out_mix[...] = signal(f_re * v_re - f_im * v_im, f_re * v_im + f_im * v_re)
    exchange(3, out_mix, got_mix)

    when_count(seq_recv.at[2], got_dif, groups - 1, groups)
    g_re, g_im = spectrum(stacked(got_dif))
    out_dv[...] = signal(f_re * g_re + f_im * g_im, f_re * g_im - f_im * g_re)
    exchange(4, out_dv, got_dv)
    out_df[...] = signal(v_re * g_re + v_im * g_im, v_re * g_im - v_im * g_re)
    exchange(5, out_df, got_df)

    @pl.when(rests)
    def _():
        take(0, [lax.rem(mc + k, rings) for k in range(1, rings)])
        gate_ref[...] = dot(weight(1, 1), full_in[...].reshape(width, tokens))
        take(1, [lax.rem(mc + k, rings) for k in range(1, rings)])
        gated_ref[...] = dot(weight(2, 1), full_grad[...].reshape(width, tokens))

    x_in = full_in[...].reshape(width, tokens)
    x_grad = full_grad[...].reshape(width, tokens)
    gate = gate_ref[...]
    d_gated = gated_ref[...]
    took(got_mix, groups - 1, seq_recv.at[3])
    mixed = by_token(got_mix[...])
    d_gate = (d_gated * mixed).astype(BF16)
    reduce_weights(gate, d_gated, d_gate, mixed, x_in, x_grad)
    from_gate = lax.dot_general(weight(1, 1), d_gate, over_first, preferred_element_type=F32)

    took(got_dv, groups - 1, seq_recv.at[4])
    d_value = by_token(got_dv[...]).astype(BF16)
    reduce_value(d_value, x_in)
    d_in = lax.dot_general(weight(0, 1), d_value, over_first, preferred_element_type=F32) + from_gate
    out_din[...] = d_in.reshape(rings, ch_rows, tokens).astype(BF16)
    for k in range(1, rings):
        block = lax.rem(mc + k, rings)
        send(out_din.at[block], got_din.at[mc], (din_send.at[0], din_recv.at[0]), me, block).start()
    got_din[mc] = out_din[mc]

    took(got_w, groups - 1, seq_recv.at[6])
    out_ws[...] = total(got_w)
    spread(7, out_ws, got_ws)
    got_ws[me] = out_ws[...]
    got_v[me] = out_v[...]

    took(got_df, groups - 1, seq_recv.at[5])
    dfil_ref[...] = by_token(got_df[...]).astype(BF16)

    took(got_v, groups - 1, seq_recv.at[8])
    dw_ref[0] = total(got_v)
    took(got_din, rings - 1, din_recv.at[0])
    din_ref[...] = total(got_din)
    took(got_ws, groups - 1, seq_recv.at[7])
    size = parts * chans
    summed = got_ws[...].astype(F32)
    dw_ref[1] = by_width(summed[:, :size, :]).astype(BF16)
    dw_ref[2] = by_width(summed[:, size:, :]).astype(BF16)

    for array in range(2):
        block_to(array, mc, other, 0).wait_send()

        @pl.when(works)
        def _():
            for s in range(1, half):
                took(wholes[array], rings - 1, line_send.at[array, 1])

        @pl.when(rests)
        def _():
            block_to(array, mc, worker, 1).wait_send()

    @pl.when(works)
    def _():
        for stage, src in ((1, out_val), (2, out_dif)):
            took(src, half * groups - 1, seq_send.at[stage])
        for s in range(1, half):
            took(weights.at[s], splits - 1, share_send.at[s])

    @pl.when(rests)
    def _():
        share_up(slot).wait_send()

    took(out_din, rings - 1, din_send.at[0])
    for stage, src in ((0, got_filt), (3, got_mix), (4, got_dv), (5, got_df), (6, got_w), (7, got_ws), (8, got_v)):
        took(src, groups - 1, seq_send.at[stage])


def finish(scale, din_ref, dw_ref, dfil_ref, din_out, dwv_out, dwg_out, dwo_out, dfil_out):
    din_out[...] = din_ref[...]
    dwv_out[...] = dw_ref[0].astype(F32) * scale
    dwg_out[...] = dw_ref[1].astype(F32) * scale
    dwo_out[...] = dw_ref[2].astype(F32) * scale
    dfil_out[...] = dfil_ref[...].astype(F32) * scale


def solution(mesh):
    groups, rings = mesh.shape["seq"], mesh.shape["ch"]

    def on_device(inputs, w_value, w_gate, w_out, filter_taps, grad_out):
        ch_rows, tokens = inputs.shape
        width = w_value.shape[0]
        chans, tiles, parts = ch_rows // groups, tokens // LANES, width // LANES
        tables = dft_tables(groups * tiles, LANES, chans)
        scale = 1.0 / math.sqrt(tokens * groups)
        vmem = pl.BlockSpec(memory_space=pltpu.VMEM)
        hbm = pl.BlockSpec(memory_space=pltpu.HBM)
        half = rings // 2
        flat = pltpu.VMEM((half * groups, tiles * chans, LANES), BF16)
        plane = pltpu.VMEM((groups, tiles * chans, LANES), BF16)
        whole = pltpu.VMEM((rings, ch_rows, tokens), BF16)
        splits = min(groups, ch_rows // 16)
        split = lambda w: w.reshape(splits, ch_rows // splits, width)
        share = pltpu.VMEM((groups, 2 * parts * chans, LANES), BF16)
        rows_of = pltpu.VMEM((ch_rows, width), BF16)
        tokens_out = jax.ShapeDtypeStruct((ch_rows, tokens), F32)
        weight_out = jax.ShapeDtypeStruct((ch_rows, width), F32)
        d_inputs, d_weights, d_filter = pl.pallas_call(
            functools.partial(body, groups, rings),
            out_shape=(
                pltpu.VMEM((ch_rows, tokens), BF16),
                pltpu.VMEM((3, ch_rows, width), BF16),
                pltpu.VMEM((ch_rows, tokens), BF16),
            ),
            in_specs=[hbm] * 11,
            out_specs=(vmem,) * 3,
            scratch_shapes=[
                whole, whole, pltpu.VMEM((ch_rows, tokens), F32), pltpu.VMEM((half, splits, 3, ch_rows // splits, width), BF16),
                plane, plane, flat, plane, flat, plane] + [plane] * 6
            + [whole, whole]
            + [share, share, pltpu.VMEM((2 * parts * chans, LANES), BF16), share, rows_of, pltpu.VMEM((groups, ch_rows, width), BF16)]
            + [pltpu.VMEM((ch_rows, tokens), F32)] * 2
            + [pltpu.VMEM(table.shape, table.dtype) for table in tables] + [
                pltpu.SemaphoreType.DMA((12,)),
                pltpu.SemaphoreType.DMA((12,)),
                pltpu.SemaphoreType.DMA((1,)),
                pltpu.SemaphoreType.DMA((1,)),
                pltpu.SemaphoreType.DMA((2, 2)),
                pltpu.SemaphoreType.DMA((2, rings)),
                pltpu.SemaphoreType.DMA((half,)),
                pltpu.SemaphoreType.DMA((half, 2)),
                pltpu.SemaphoreType.DMA((5,)),
                pltpu.SemaphoreType.DMA((6,)),
                pltpu.SemaphoreType.REGULAR((len(near(groups)) + half - 2,)),
            ],
            compiler_params=pltpu.CompilerParams(collective_id=0, has_side_effects=True),
        )(
            inputs, split(w_value.T), split(w_gate.T), split(w_out), filter_taps, grad_out, *tables,
        )
        d_inputs, d_w_value, d_w_gate, d_w_out, d_filter = pl.pallas_call(
            functools.partial(finish, scale),
            out_shape=(
                jax.ShapeDtypeStruct((ch_rows, tokens), BF16), weight_out, weight_out, weight_out, tokens_out,
            ),
            in_specs=[vmem] * 3,
            out_specs=(vmem,) * 5,
            compiler_params=pltpu.CompilerParams(vmem_limit_bytes=8 << 20),
        )(d_inputs, d_weights, d_filter)
        return d_inputs, d_w_value.T, d_w_gate.T, d_w_out, d_filter

    return jax.shard_map(
        on_device,
        mesh=mesh,
        in_specs=(P("ch", "seq"), P(None, "ch"), P(None, "ch"), P("ch", None), P("ch", "seq"), P("ch", "seq")),
        out_specs=(P("ch", "seq"), P(None, "ch"), P(None, "ch"), P("ch", None), P("ch", "seq")),
        check_vma=False,
    )
```

```python
import functools
import math

import jax
import jax.numpy as jnp
import numpy as np
from jax import lax
from jax.experimental import pallas as pl
from jax.experimental.pallas import tpu as pltpu
from jax.sharding import PartitionSpec as P

F32 = jnp.float32
BF16 = jnp.bfloat16
LANES = 128


def dft_tables(strides, lanes, chans):
    length = 2 * strides * lanes
    n1 = np.arange(strides)
    n2 = np.arange(lanes)
    half = np.arange(strides) + 0.5
    first = np.exp(-2j * np.pi * np.outer(half, n1) / (2 * strides))
    eye = np.eye(chans)
    first_re, first_im = np.kron(first.real, eye), np.kron(first.imag, eye)
    ahead = np.concatenate([first_re, first_im], 0)
    twist = np.repeat(np.exp(-2j * np.pi * np.outer(half, n2) / length), chans, axis=0)
    last = np.exp(-2j * np.pi * np.outer(n2, n2) / lanes)
    c, s = last.real, last.imag
    across = np.block([[c, s], [-s, c]])
    low = lambda a: jnp.asarray(a.astype(np.float32)).astype(BF16)
    wide = lambda a: jnp.asarray(a.astype(np.float32))
    return (
        low(ahead),
        low(ahead.T * (2.0 / length)),
        low(across),
        low(across.T),
        wide(np.stack([twist.real, twist.imag])),
    )


def each(count, step):
    if count <= 16:
        for k in range(count):
            step(k)
    else:
        lax.fori_loop(0, count, lambda k, carry: (step(k), carry)[1], 0)


def near(count):
    return [1 << b for b in range(count.bit_length() - 1)]


def body(
    groups, rings,
    in_hbm, wv_hbm, wg_hbm, wo_hbm, filt_hbm, grad_hbm, ahead_hbm, back_hbm, across_hbm, return_hbm, twist_hbm,
    din_ref, dw_ref, dfil_ref,
    full_in, full_grad, filt_ref, weights, out_filt, got_filt, out_val, got_val, out_dif, got_dif,
    out_mix, got_mix, out_dv, got_dv, out_df, got_df,
    out_din, got_din, out_w, got_w, out_ws, got_ws, out_v, got_v, gate_ref, gated_ref,
    ahead_ref, back_ref, across_ref, return_ref, twist_ref,
    seq_send, seq_recv, din_send, din_recv, line_send, line_recv, share_send, share_recv,
    table_sem, fetch_sem, round_sem,
):
    me = lax.axis_index("seq")
    mc = lax.axis_index("ch")
    ch_rows, tokens = in_hbm.shape
    chans = ch_rows // groups
    tiles = tokens // LANES
    width = full_in.shape[0] * ch_rows
    parts = width // LANES
    half = rings // 2
    splits = weights.shape[1]
    right = lax.div(mc, half)
    toward = 1 - 2 * right
    worker = half - 1 + right
    other = half - right
    slot = (worker - mc) * toward
    works = slot == 0
    rests = slot > 0
    between = (mc > 0) & (mc < rings - 1)
    barrier = pltpu.get_barrier_semaphore()
    hops = near(groups)

    def can(step):
        return mc < rings - 1 if step == 1 else mc > 0

    def greet(semaphore):
        for step in (1, -1):
            @pl.when(can(step))
            def _():
                pl.semaphore_signal(
                    semaphore, inc=1, device_id={"ch": mc + step}, device_id_type=pl.DeviceIdType.MESH)
        for hop_by in hops:
            pl.semaphore_signal(
                semaphore, inc=1, device_id={"seq": me ^ hop_by}, device_id_type=pl.DeviceIdType.MESH)

    def greeted(semaphore):
        @pl.when(between)
        def _():
            pl.semaphore_wait(semaphore, len(hops) + 2)

        @pl.when(jnp.logical_not(between))
        def _():
            pl.semaphore_wait(semaphore, len(hops) + 1)

    greet(barrier)
    fetches = [
        pltpu.make_async_copy(src, dst, fetch_sem.at[i])
        for i, (src, dst) in enumerate((
            (in_hbm, full_in.at[mc]), (grad_hbm, full_grad.at[mc]),
            (wv_hbm, weights.at[0, :, 0]), (wg_hbm, weights.at[0, :, 1]), (wo_hbm, weights.at[0, :, 2]),
            (filt_hbm, filt_ref)))
    ]
    tables = [
        pltpu.make_async_copy(src, dst, table_sem.at[i])
        for i, (src, dst) in enumerate((
            (ahead_hbm, ahead_ref), (twist_hbm, twist_ref), (across_hbm, across_ref),
            (return_hbm, return_ref), (back_hbm, back_ref)))
    ]
    for copy in fetches:
        copy.start()

    for copy in tables:
        copy.start()

    greeted(barrier)

    def send(src, dst, sems, seq, ch):
        return pltpu.make_async_remote_copy(
            src_ref=src, dst_ref=dst, send_sem=sems[0], recv_sem=sems[1],
            device_id={"seq": seq, "ch": ch}, device_id_type=pl.DeviceIdType.MESH)

    def stage_sems(stage):
        return seq_send.at[stage], seq_recv.at[stage]

    def seq_peer(k):
        return lax.rem(me + k, groups)

    def took(ref, count, semaphore):
        blocks = ref.at[pl.ds(0, count)]
        pltpu.make_async_copy(blocks, blocks, semaphore).wait()

    def scatter(stage, src, dst, ch, skip, base=0):
        each(groups - skip, lambda k: send(
            src.at[base + (me ^ (groups - 1 - k))], dst, stage_sems(stage), me ^ (groups - 1 - k), ch).start())

    def spread(stage, src, dst):
        each(groups - 1, lambda k: send(
            src, dst.at[me], stage_sems(stage), me ^ (groups - 1 - k), mc).start())

    def to_plane(stage, src, dst, s):
        scatter(stage, src, dst.at[me], mc - toward * s, 1 if s == 0 else 0, s * groups)
        if s == 0:
            dst[me] = src[me]

    def to_planes(stage, src, dst):
        for s in range(half):
            scatter(stage, src, dst.at[me], mc - toward * s, 1 if s == 0 else 0, s * groups)
        dst[me] = src[me]

    wholes = (full_in, full_grad)

    def block_to(array, block, ch, k):
        return send(
            wholes[array].at[block], wholes[array].at[block],
            (line_send.at[array, k], line_recv.at[array, block]), me, ch)

    def take(array, blocks):
        for block in blocks:
            block_to(array, block, mc, 0).wait_recv()

    def pass_on(array, block):
        for s in range(1, half):
            block_to(array, block, mc - toward * s, 1).start()

    def pass_inner(array):
        for s in range(1, half):
            for t in range(1, half):
                if t != s:
                    block_to(array, mc - toward * t, mc - toward * s, 1).start()

    far_blocks = [other + toward * k for k in range(1, half)]
    outer_blocks = [mc - toward * k for k in range(1, half)]

    mine = lax.rem(me, splits)

    def share_up(s):
        return send(weights.at[0, mine], weights.at[s, mine], (share_send.at[0], share_recv.at[s, 0]), me, worker)

    def share_across(s, k):
        return send(
            weights.at[s, mine], weights.at[s, mine], (share_send.at[s], share_recv.at[s, 1]), me ^ k, mc)

    for kind in range(3):
        fetches[2 + kind].wait()

    @pl.when(rests)
    def _():
        share_up(slot).start()

    for array in range(2):
        fetches[array].wait()

        @pl.when(works)
        def _():
            block_to(array, mc, other, 0).start()

        @pl.when(rests)
        def _():
            block_to(array, mc, worker, 1).start()

    for turn in range(len(hops) + half - 2):
        greet(round_sem.at[turn])
        greeted(round_sem.at[turn])
        if turn == half - 2:
            for array in range(2):
                @pl.when(works)
                def _():
                    for s in range(1, half):
                        block_to(array, mc, mc - toward * s, 1).start()

                @pl.when(rests)
                def _():
                    block_to(array, mc, other, 0).start()

    def by_owner(x):
        x = x.reshape(groups, chans, tokens)
        return jnp.concatenate([x[:, :, j * LANES:(j + 1) * LANES] for j in range(tiles)], axis=1).astype(BF16)

    def by_token(x):
        x = x.astype(F32)
        x = jnp.concatenate([x[:, j * chans:(j + 1) * chans, :] for j in range(tiles)], axis=2)
        return x.reshape(ch_rows, tokens)

    fetches[5].wait()
    out_filt[...] = by_owner(filt_ref[...])

    scatter(0, out_filt, got_filt.at[me], mc, 1)
    got_filt[me] = out_filt[me]

    @pl.when(works)
    def _():
        for s in range(1, half):
            share_up(s).wait_recv()
            for k in range(1, splits):
                share_across(s, k).start()

    def by_share(x):
        x = x.reshape(groups, chans, width)
        return jnp.concatenate([x[:, :, j * LANES:(j + 1) * LANES] for j in range(parts)], axis=1)

    def by_width(x):
        return jnp.concatenate([x[:, j * chans:(j + 1) * chans, :] for j in range(parts)], axis=2).reshape(ch_rows, width)

    def total(ref):
        out = ref[0].astype(F32)
        for p in range(1, ref.shape[0]):
            out = out + ref[p].astype(F32)
        return out.astype(BF16)

    rows = ahead_ref.shape[1]

    def dot(a, b):
        return jnp.dot(a, b, preferred_element_type=F32)

    def spectrum(x):
        first = dot(ahead_ref[...], x)
        re, im = first[:rows], first[rows:]
        tw_re, tw_im = twist_ref[0], twist_ref[1]
        mid = jnp.concatenate([re * tw_re - im * tw_im, re * tw_im + im * tw_re], axis=1).astype(BF16)
        out = dot(mid, across_ref[...])
        return out[:, :LANES], out[:, LANES:]

    def signal(re, im):
        mid = dot(jnp.concatenate([re, im], axis=1).astype(BF16), return_ref[...])
        re, im = mid[:, :LANES], mid[:, LANES:]
        tw_re, tw_im = twist_ref[0], twist_ref[1]
        tall = jnp.concatenate([re * tw_re + im * tw_im, im * tw_re - re * tw_im], axis=0).astype(BF16)
        return dot(back_ref[...], tall).reshape(groups, tiles * chans, LANES).astype(BF16)

    def slots(x):
        size = x.shape[0] // half
        return [x[s * size:(s + 1) * size] for s in range(half)]

    def stacked(ref):
        return jnp.concatenate([ref[p] for p in range(groups)], axis=0)

    def put_flat(ref, xs):
        for s in range(half):
            ref[s * groups:(s + 1) * groups] = xs[s]

    def exchange(stage, src, dst):
        scatter(stage, src, dst.at[me], mc, 1)
        dst[me] = src[me]

    def weight(kind, count):
        return jnp.concatenate([weights[s, q, kind] for s in range(count) for q in range(splits)], axis=0)

    def weight_of(kind, s):
        return jnp.concatenate([weights[s, q, kind] for q in range(splits)], axis=0)

    def reduce_weights(gate, d_gated, d_gate, mixed, x_in, x_grad):
        gated_out = (gate[:ch_rows] * mixed[:ch_rows]).astype(BF16)
        gate_term = lax.dot_general(d_gate[:ch_rows], x_in, over_last, preferred_element_type=F32)
        out_term = lax.dot_general(gated_out, x_grad, over_last, preferred_element_type=F32)
        out_w[...] = jnp.concatenate([by_share(gate_term), by_share(out_term)], axis=1).astype(BF16)
        exchange(6, out_w, got_w)

    def reduce_value(d_value, x_in):
        value_term = lax.dot_general(d_value[:ch_rows], x_in, over_last, preferred_element_type=F32)
        out_v[...] = value_term.astype(BF16)
        spread(8, out_v, got_v)

    over_first = (((0,), (0,)), ((), ()))
    over_last = (((1,), (1,)), ((), ()))

    def when_count(semaphore, ref, working, resting):
        @pl.when(works)
        def _():
            took(ref, working, semaphore)

        @pl.when(rests)
        def _():
            took(ref, resting, semaphore)

    @pl.when(works)
    def _():
        for array in range(2):
            take(array, [other])
            pass_on(array, other)
        take(0, outer_blocks + far_blocks)
        for s in range(1, half):
            across = weights.at[s, pl.ds(0, splits - 1)]
            pltpu.make_async_copy(across, across, share_recv.at[s, 1]).wait()
        x_in = full_in[...].reshape(width, tokens)
        order = list(reversed(range(half)))
        for s in order:
            out_val[s * groups:(s + 1) * groups] = by_owner(dot(weight_of(0, s), x_in))
            to_plane(1, out_val, got_val, s)
        gates = {s: dot(weight_of(1, s), x_in) for s in order}
        gate_ref[...] = gates[0]
        take(1, outer_blocks + far_blocks)
        x_grad = full_grad[...].reshape(width, tokens)
        for s in order:
            d_gated = dot(weight_of(2, s), x_grad)
            out_dif[s * groups:(s + 1) * groups] = by_owner(d_gated * gates[s])
            to_plane(2, out_dif, got_dif, s)
            if s == 0:
                gated_ref[...] = d_gated
        for array in range(2):
            for block in far_blocks:
                pass_on(array, block)
            pass_inner(array)

    for table in tables:
        table.wait()
    took(got_filt, groups - 1, seq_recv.at[0])
    f_re, f_im = spectrum(stacked(got_filt))
    when_count(seq_recv.at[1], got_val, groups - 1, groups)
    v_re, v_im = spectrum(stacked(got_val))
    out_mix[...] = signal(f_re * v_re - f_im * v_im, f_re * v_im + f_im * v_re)
    exchange(3, out_mix, got_mix)

    when_count(seq_recv.at[2], got_dif, groups - 1, groups)
    g_re, g_im = spectrum(stacked(got_dif))
    out_dv[...] = signal(f_re * g_re + f_im * g_im, f_re * g_im - f_im * g_re)
    exchange(4, out_dv, got_dv)
    out_df[...] = signal(v_re * g_re + v_im * g_im, v_re * g_im - v_im * g_re)
    exchange(5, out_df, got_df)

    @pl.when(rests)
    def _():
        take(0, [lax.rem(mc + k, rings) for k in range(1, rings)])
        gate_ref[...] = dot(weight(1, 1), full_in[...].reshape(width, tokens))
        take(1, [lax.rem(mc + k, rings) for k in range(1, rings)])
        gated_ref[...] = dot(weight(2, 1), full_grad[...].reshape(width, tokens))

    x_in = full_in[...].reshape(width, tokens)
    x_grad = full_grad[...].reshape(width, tokens)
    gate = gate_ref[...]
    d_gated = gated_ref[...]
    took(got_mix, groups - 1, seq_recv.at[3])
    mixed = by_token(got_mix[...])
    d_gate = (d_gated * mixed).astype(BF16)
    reduce_weights(gate, d_gated, d_gate, mixed, x_in, x_grad)
    from_gate = lax.dot_general(weight(1, 1), d_gate, over_first, preferred_element_type=F32)

    took(got_dv, groups - 1, seq_recv.at[4])
    d_value = by_token(got_dv[...]).astype(BF16)
    reduce_value(d_value, x_in)
    d_in = lax.dot_general(weight(0, 1), d_value, over_first, preferred_element_type=F32) + from_gate
    out_din[...] = d_in.reshape(rings, ch_rows, tokens).astype(BF16)
    for k in range(1, rings):
        block = lax.rem(mc + k, rings)
        send(out_din.at[block], got_din.at[mc], (din_send.at[0], din_recv.at[0]), me, block).start()
    got_din[mc] = out_din[mc]

    took(got_w, groups - 1, seq_recv.at[6])
    out_ws[...] = total(got_w)
    spread(7, out_ws, got_ws)
    got_ws[me] = out_ws[...]
    got_v[me] = out_v[...]

    took(got_df, groups - 1, seq_recv.at[5])
    dfil_ref[...] = by_token(got_df[...]).astype(BF16)

    took(got_v, groups - 1, seq_recv.at[8])
    dw_ref[0] = total(got_v)
    took(got_din, rings - 1, din_recv.at[0])
    din_ref[...] = total(got_din)
    took(got_ws, groups - 1, seq_recv.at[7])
    size = parts * chans
    summed = got_ws[...].astype(F32)
    dw_ref[1] = by_width(summed[:, :size, :]).astype(BF16)
    dw_ref[2] = by_width(summed[:, size:, :]).astype(BF16)

    for array in range(2):
        block_to(array, mc, other, 0).wait_send()

        @pl.when(works)
        def _():
            for s in range(1, half):
                took(wholes[array], rings - 1, line_send.at[array, 1])

        @pl.when(rests)
        def _():
            block_to(array, mc, worker, 1).wait_send()

    @pl.when(works)
    def _():
        for stage, src in ((1, out_val), (2, out_dif)):
            took(src, half * groups - 1, seq_send.at[stage])
        for s in range(1, half):
            took(weights.at[s], splits - 1, share_send.at[s])

    @pl.when(rests)
    def _():
        share_up(slot).wait_send()

    took(out_din, rings - 1, din_send.at[0])
    for stage, src in ((0, got_filt), (3, got_mix), (4, got_dv), (5, got_df), (6, got_w), (7, got_ws), (8, got_v)):
        took(src, groups - 1, seq_send.at[stage])


def finish(scale, din_ref, dw_ref, dfil_ref, din_out, dwv_out, dwg_out, dwo_out, dfil_out):
    din_out[...] = din_ref[...]
    dwv_out[...] = dw_ref[0].astype(F32) * scale
    dwg_out[...] = dw_ref[1].astype(F32) * scale
    dwo_out[...] = dw_ref[2].astype(F32) * scale
    dfil_out[...] = dfil_ref[...].astype(F32) * scale


def solution(mesh):
    groups, rings = mesh.shape["seq"], mesh.shape["ch"]

    def on_device(inputs, w_value, w_gate, w_out, filter_taps, grad_out):
        ch_rows, tokens = inputs.shape
        width = w_value.shape[0]
        chans, tiles, parts = ch_rows // groups, tokens // LANES, width // LANES
        tables = dft_tables(groups * tiles, LANES, chans)
        scale = 1.0 / math.sqrt(tokens * groups)
        vmem = pl.BlockSpec(memory_space=pltpu.VMEM)
        hbm = pl.BlockSpec(memory_space=pltpu.HBM)
        half = rings // 2
        flat = pltpu.VMEM((half * groups, tiles * chans, LANES), BF16)
        plane = pltpu.VMEM((groups, tiles * chans, LANES), BF16)
        whole = pltpu.VMEM((rings, ch_rows, tokens), BF16)
        splits = min(groups, ch_rows // 16)
        split = lambda w: w.reshape(splits, ch_rows // splits, width)
        share = pltpu.VMEM((groups, 2 * parts * chans, LANES), BF16)
        rows_of = pltpu.VMEM((ch_rows, width), BF16)
        tokens_out = jax.ShapeDtypeStruct((ch_rows, tokens), F32)
        weight_out = jax.ShapeDtypeStruct((ch_rows, width), F32)
        d_inputs, d_weights, d_filter = pl.pallas_call(
            functools.partial(body, groups, rings),
            out_shape=(
                pltpu.VMEM((ch_rows, tokens), BF16),
                pltpu.VMEM((3, ch_rows, width), BF16),
                pltpu.VMEM((ch_rows, tokens), BF16),
            ),
            in_specs=[hbm] * 11,
            out_specs=(vmem,) * 3,
            scratch_shapes=[
                whole, whole, pltpu.VMEM((ch_rows, tokens), F32), pltpu.VMEM((half, splits, 3, ch_rows // splits, width), BF16),
                plane, plane, flat, plane, flat, plane] + [plane] * 6
            + [whole, whole]
            + [share, share, pltpu.VMEM((2 * parts * chans, LANES), BF16), share, rows_of, pltpu.VMEM((groups, ch_rows, width), BF16)]
            + [pltpu.VMEM((ch_rows, tokens), F32)] * 2
            + [pltpu.VMEM(table.shape, table.dtype) for table in tables] + [
                pltpu.SemaphoreType.DMA((12,)),
                pltpu.SemaphoreType.DMA((12,)),
                pltpu.SemaphoreType.DMA((1,)),
                pltpu.SemaphoreType.DMA((1,)),
                pltpu.SemaphoreType.DMA((2, 2)),
                pltpu.SemaphoreType.DMA((2, rings)),
                pltpu.SemaphoreType.DMA((half,)),
                pltpu.SemaphoreType.DMA((half, 2)),
                pltpu.SemaphoreType.DMA((5,)),
                pltpu.SemaphoreType.DMA((6,)),
                pltpu.SemaphoreType.REGULAR((len(near(groups)) + half - 2,)),
            ],
            compiler_params=pltpu.CompilerParams(collective_id=0, has_side_effects=True),
        )(
            inputs, split(w_value.T), split(w_gate.T), split(w_out), filter_taps, grad_out, *tables,
        )
        d_inputs, d_w_value, d_w_gate, d_w_out, d_filter = pl.pallas_call(
            functools.partial(finish, scale),
            out_shape=(
                jax.ShapeDtypeStruct((ch_rows, tokens), BF16), weight_out, weight_out, weight_out, tokens_out,
            ),
            in_specs=[vmem] * 3,
            out_specs=(vmem,) * 5,
            compiler_params=pltpu.CompilerParams(vmem_limit_bytes=8 << 20),
        )(d_inputs, d_weights, d_filter)
        return d_inputs, d_w_value.T, d_w_gate.T, d_w_out, d_filter

    return jax.shard_map(
        on_device,
        mesh=mesh,
        in_specs=(P("ch", "seq"), P(None, "ch"), P(None, "ch"), P("ch", None), P("ch", "seq"), P("ch", "seq")),
        out_specs=(P("ch", "seq"), P(None, "ch"), P(None, "ch"), P("ch", None), P("ch", "seq")),
        check_vma=False,
    )
```

```python
import functools
import math

import jax
import jax.numpy as jnp
import numpy as np
from jax import lax
from jax.experimental import pallas as pl
from jax.experimental.pallas import tpu as pltpu
from jax.sharding import PartitionSpec as P

F32 = jnp.float32
BF16 = jnp.bfloat16
LANES = 128


def dft_tables(strides, lanes, chans):
    length = 2 * strides * lanes
    n1 = np.arange(strides)
    n2 = np.arange(lanes)
    half = np.arange(strides) + 0.5
    first = np.exp(-2j * np.pi * np.outer(half, n1) / (2 * strides))
    eye = np.eye(chans)
    first_re, first_im = np.kron(first.real, eye), np.kron(first.imag, eye)
    ahead = np.concatenate([first_re, first_im], 0)
    twist = np.repeat(np.exp(-2j * np.pi * np.outer(half, n2) / length), chans, axis=0)
    last = np.exp(-2j * np.pi * np.outer(n2, n2) / lanes)
    c, s = last.real, last.imag
    across = np.block([[c, s], [-s, c]])
    low = lambda a: jnp.asarray(a.astype(np.float32)).astype(BF16)
    wide = lambda a: jnp.asarray(a.astype(np.float32))
    return (
        low(ahead),
        low(ahead.T * (2.0 / length)),
        low(across),
        low(across.T),
        wide(np.stack([twist.real, twist.imag])),
    )


def each(count, step):
    if count <= 16:
        for k in range(count):
            step(k)
    else:
        lax.fori_loop(0, count, lambda k, carry: (step(k), carry)[1], 0)


def near(count):
    return [1 << b for b in range(count.bit_length() - 1)]


def body(
    groups, rings,
    in_hbm, wv_hbm, wg_hbm, wo_hbm, filt_hbm, grad_hbm, ahead_hbm, back_hbm, across_hbm, return_hbm, twist_hbm,
    din_ref, dw_ref, dfil_ref,
    full_in, full_grad, filt_ref, weights, out_filt, got_filt, out_val, got_val, out_dif, got_dif,
    out_mix, got_mix, out_dv, got_dv, out_df, got_df,
    out_din, got_din, out_w, got_w, out_ws, got_ws, out_v, got_v, pair_ref, sum_ref, gate_ref, gated_ref,
    ahead_ref, back_ref, across_ref, return_ref, twist_ref,
    seq_send, seq_recv, din_send, din_recv, line_send, line_recv, share_send, share_recv,
    table_sem, fetch_sem, round_sem,
):
    me = lax.axis_index("seq")
    mc = lax.axis_index("ch")
    ch_rows, tokens = in_hbm.shape
    chans = ch_rows // groups
    tiles = tokens // LANES
    width = full_in.shape[0] * ch_rows
    parts = width // LANES
    half = rings // 2
    splits = weights.shape[1]
    right = lax.div(mc, half)
    toward = 1 - 2 * right
    worker = half - 1 + right
    other = half - right
    slot = (worker - mc) * toward
    works = slot == 0
    rests = slot > 0
    between = (mc > 0) & (mc < rings - 1)
    core = lax.rem(me, 2)
    barrier = pltpu.get_barrier_semaphore()
    hops = near(groups)

    def can(step):
        return mc < rings - 1 if step == 1 else mc > 0

    def greet(semaphore):
        for step in (1, -1):
            @pl.when(can(step))
            def _():
                pl.semaphore_signal(
                    semaphore, inc=1, device_id={"ch": mc + step}, device_id_type=pl.DeviceIdType.MESH)
        for hop_by in hops:
            pl.semaphore_signal(
                semaphore, inc=1, device_id={"seq": me ^ hop_by}, device_id_type=pl.DeviceIdType.MESH)

    def greeted(semaphore):
        @pl.when(between)
        def _():
            pl.semaphore_wait(semaphore, len(hops) + 2)

        @pl.when(jnp.logical_not(between))
        def _():
            pl.semaphore_wait(semaphore, len(hops) + 1)

    greet(barrier)
    fetches = [
        pltpu.make_async_copy(src, dst, fetch_sem.at[i])
        for i, (src, dst) in enumerate((
            (in_hbm, full_in.at[mc]), (grad_hbm, full_grad.at[mc]),
            (wv_hbm, weights.at[0, :, 0]), (wg_hbm, weights.at[0, :, 1]), (wo_hbm, weights.at[0, :, 2]),
            (filt_hbm, filt_ref)))
    ]
    tables = [
        pltpu.make_async_copy(src, dst, table_sem.at[i])
        for i, (src, dst) in enumerate((
            (ahead_hbm, ahead_ref), (twist_hbm, twist_ref), (across_hbm, across_ref),
            (return_hbm, return_ref), (back_hbm, back_ref)))
    ]
    for copy in fetches:
        copy.start()

    for copy in tables:
        copy.start()

    greeted(barrier)

    def send(src, dst, sems, seq, ch):
        return pltpu.make_async_remote_copy(
            src_ref=src, dst_ref=dst, send_sem=sems[0], recv_sem=sems[1],
            device_id={"seq": seq, "ch": ch}, device_id_type=pl.DeviceIdType.MESH)

    def stage_sems(stage):
        return seq_send.at[stage], seq_recv.at[stage]

    def seq_peer(k):
        return lax.rem(me + k, groups)

    def took(ref, count, semaphore):
        blocks = ref.at[pl.ds(0, count)]
        pltpu.make_async_copy(blocks, blocks, semaphore).wait()

    def scatter(stage, src, dst, ch, skip, base=0):
        each(groups - skip, lambda k: send(
            src.at[base + (me ^ (groups - 1 - k))], dst, stage_sems(stage), me ^ (groups - 1 - k), ch).start())

    def spread(stage, src, dst):
        each(groups - 1, lambda k: send(
            src, dst.at[me], stage_sems(stage), me ^ (groups - 1 - k), mc).start())

    def to_plane(stage, src, dst, s):
        scatter(stage, src, dst.at[me], mc - toward * s, 1 if s == 0 else 0, s * groups)
        if s == 0:
            dst[me] = src[me]

    def to_planes(stage, src, dst):
        for s in range(half):
            scatter(stage, src, dst.at[me], mc - toward * s, 1 if s == 0 else 0, s * groups)
        dst[me] = src[me]

    wholes = (full_in, full_grad)

    def block_to(array, block, ch, k):
        return send(
            wholes[array].at[block], wholes[array].at[block],
            (line_send.at[array, k], line_recv.at[array, block]), me, ch)

    def take(array, blocks):
        for block in blocks:
            block_to(array, block, mc, 0).wait_recv()

    def pass_on(array, block):
        for s in range(1, half):
            block_to(array, block, mc - toward * s, 1).start()

    def pass_inner(array):
        for s in range(1, half):
            for t in range(1, half):
                if t != s:
                    block_to(array, mc - toward * t, mc - toward * s, 1).start()

    far_blocks = [other + toward * k for k in range(1, half)]
    outer_blocks = [mc - toward * k for k in range(1, half)]

    mine = lax.rem(me, splits)

    def share_up(s):
        return send(weights.at[0, mine], weights.at[s, mine], (share_send.at[0], share_recv.at[s, 0]), me, worker)

    def share_across(s, k):
        return send(
            weights.at[s, mine], weights.at[s, mine], (share_send.at[s], share_recv.at[s, 1]), me ^ k, mc)

    for kind in range(3):
        fetches[2 + kind].wait()

    @pl.when(rests)
    def _():
        share_up(slot).start()

    for array in range(2):
        fetches[array].wait()

        @pl.when(works)
        def _():
            block_to(array, mc, other, 0).start()

        @pl.when(rests)
        def _():
            block_to(array, mc, worker, 1).start()

    for turn in range(len(hops) + half - 2):
        greet(round_sem.at[turn])
        greeted(round_sem.at[turn])
        if turn == half - 2:
            for array in range(2):
                @pl.when(works)
                def _():
                    for s in range(1, half):
                        block_to(array, mc, mc - toward * s, 1).start()

                @pl.when(rests)
                def _():
                    block_to(array, mc, other, 0).start()

    def by_owner(x):
        x = x.reshape(groups, chans, tokens)
        return jnp.concatenate([x[:, :, j * LANES:(j + 1) * LANES] for j in range(tiles)], axis=1).astype(BF16)

    def by_token(x):
        x = x.astype(F32)
        x = jnp.concatenate([x[:, j * chans:(j + 1) * chans, :] for j in range(tiles)], axis=2)
        return x.reshape(ch_rows, tokens)

    fetches[5].wait()
    out_filt[...] = by_owner(filt_ref[...])

    scatter(0, out_filt, got_filt.at[me], mc, 1)
    got_filt[me] = out_filt[me]

    @pl.when(works)
    def _():
        for s in range(1, half):
            share_up(s).wait_recv()
            for k in range(1, splits):
                share_across(s, k).start()

    def by_share(x):
        x = x.reshape(groups, chans, width)
        return jnp.concatenate([x[:, :, j * LANES:(j + 1) * LANES] for j in range(parts)], axis=1)

    def by_width(x):
        return jnp.concatenate([x[:, j * chans:(j + 1) * chans, :] for j in range(parts)], axis=2).reshape(ch_rows, width)

    def total(ref):
        out = ref[0].astype(F32)
        for p in range(1, ref.shape[0]):
            out = out + ref[p].astype(F32)
        return out.astype(BF16)

    rows = ahead_ref.shape[1]

    def dot(a, b):
        return jnp.dot(a, b, preferred_element_type=F32)

    def spectrum(x):
        first = dot(ahead_ref[...], x)
        re, im = first[:rows], first[rows:]
        tw_re, tw_im = twist_ref[0], twist_ref[1]
        mid = jnp.concatenate([re * tw_re - im * tw_im, re * tw_im + im * tw_re], axis=1).astype(BF16)
        out = dot(mid, across_ref[...])
        return out[:, :LANES], out[:, LANES:]

    def signal(re, im):
        mid = dot(jnp.concatenate([re, im], axis=1).astype(BF16), return_ref[...])
        re, im = mid[:, :LANES], mid[:, LANES:]
        tw_re, tw_im = twist_ref[0], twist_ref[1]
        tall = jnp.concatenate([re * tw_re + im * tw_im, im * tw_re - re * tw_im], axis=0).astype(BF16)
        return dot(back_ref[...], tall).reshape(groups, tiles * chans, LANES).astype(BF16)

    def slots(x):
        size = x.shape[0] // half
        return [x[s * size:(s + 1) * size] for s in range(half)]

    def stacked(ref):
        return jnp.concatenate([ref[p] for p in range(groups)], axis=0)

    def put_flat(ref, xs):
        for s in range(half):
            ref[s * groups:(s + 1) * groups] = xs[s]

    def exchange(stage, src, dst):
        scatter(stage, src, dst.at[me], mc, 1)
        dst[me] = src[me]

    def weight(kind, count):
        return jnp.concatenate([weights[s, q, kind] for s in range(count) for q in range(splits)], axis=0)

    def weight_of(kind, s):
        return jnp.concatenate([weights[s, q, kind] for q in range(splits)], axis=0)

    def reduce_weights(gate, d_gated, d_gate, mixed, x_in, x_grad):
        gated_out = (gate[:ch_rows] * mixed[:ch_rows]).astype(BF16)
        gate_term = lax.dot_general(d_gate[:ch_rows], x_in, over_last, preferred_element_type=F32)
        out_term = lax.dot_general(gated_out, x_grad, over_last, preferred_element_type=F32)
        out_w[...] = jnp.concatenate([by_share(gate_term), by_share(out_term)], axis=1).astype(BF16)
        exchange(6, out_w, got_w)

    def pair_copy():
        return send(
            out_v.at[1 - core], pair_ref, stage_sems(9), me ^ 1, mc)

    def reduce_value(d_value, x_in):
        value_term = lax.dot_general(d_value[:ch_rows], x_in, over_last, preferred_element_type=F32)
        out_v[...] = value_term.reshape(2, ch_rows // 2, width).astype(BF16)
        pair_copy().start()

    def spread_value():
        pair_copy().wait_recv()
        sum_ref[...] = (out_v[core].astype(F32) + pair_ref[...].astype(F32)).astype(BF16)
        spread(8, sum_ref, got_v)
        got_v[me] = sum_ref[...]

    over_first = (((0,), (0,)), ((), ()))
    over_last = (((1,), (1,)), ((), ()))

    def when_count(semaphore, ref, working, resting):
        @pl.when(works)
        def _():
            took(ref, working, semaphore)

        @pl.when(rests)
        def _():
            took(ref, resting, semaphore)

    @pl.when(works)
    def _():
        for array in range(2):
            take(array, [other])
            pass_on(array, other)
        take(0, outer_blocks + far_blocks)
        for s in range(1, half):
            across = weights.at[s, pl.ds(0, splits - 1)]
            pltpu.make_async_copy(across, across, share_recv.at[s, 1]).wait()
        x_in = full_in[...].reshape(width, tokens)
        order = list(reversed(range(half)))
        for s in order:
            out_val[s * groups:(s + 1) * groups] = by_owner(dot(weight_of(0, s), x_in))
            to_plane(1, out_val, got_val, s)
        gates = {s: dot(weight_of(1, s), x_in) for s in order}
        gate_ref[...] = gates[0]
        take(1, outer_blocks + far_blocks)
        x_grad = full_grad[...].reshape(width, tokens)
        for s in order:
            d_gated = dot(weight_of(2, s), x_grad)
            out_dif[s * groups:(s + 1) * groups] = by_owner(d_gated * gates[s])
            to_plane(2, out_dif, got_dif, s)
            if s == 0:
                gated_ref[...] = d_gated
        for array in range(2):
            for block in far_blocks:
                pass_on(array, block)
            pass_inner(array)

    for table in tables:
        table.wait()
    took(got_filt, groups - 1, seq_recv.at[0])
    f_re, f_im = spectrum(stacked(got_filt))
    when_count(seq_recv.at[1], got_val, groups - 1, groups)
    v_re, v_im = spectrum(stacked(got_val))
    out_mix[...] = signal(f_re * v_re - f_im * v_im, f_re * v_im + f_im * v_re)
    exchange(3, out_mix, got_mix)

    when_count(seq_recv.at[2], got_dif, groups - 1, groups)
    g_re, g_im = spectrum(stacked(got_dif))
    out_dv[...] = signal(f_re * g_re + f_im * g_im, f_re * g_im - f_im * g_re)
    exchange(4, out_dv, got_dv)
    out_df[...] = signal(v_re * g_re + v_im * g_im, v_re * g_im - v_im * g_re)
    exchange(5, out_df, got_df)

    @pl.when(rests)
    def _():
        take(0, [lax.rem(mc + k, rings) for k in range(1, rings)])
        gate_ref[...] = dot(weight(1, 1), full_in[...].reshape(width, tokens))
        take(1, [lax.rem(mc + k, rings) for k in range(1, rings)])
        gated_ref[...] = dot(weight(2, 1), full_grad[...].reshape(width, tokens))

    x_in = full_in[...].reshape(width, tokens)
    x_grad = full_grad[...].reshape(width, tokens)
    gate = gate_ref[...]
    d_gated = gated_ref[...]
    took(got_mix, groups - 1, seq_recv.at[3])
    mixed = by_token(got_mix[...])
    d_gate = (d_gated * mixed).astype(BF16)
    reduce_weights(gate, d_gated, d_gate, mixed, x_in, x_grad)
    from_gate = lax.dot_general(weight(1, 1), d_gate, over_first, preferred_element_type=F32)

    took(got_dv, groups - 1, seq_recv.at[4])
    d_value = by_token(got_dv[...]).astype(BF16)
    reduce_value(d_value, x_in)
    d_in = lax.dot_general(weight(0, 1), d_value, over_first, preferred_element_type=F32) + from_gate
    out_din[...] = d_in.reshape(rings, ch_rows, tokens).astype(BF16)
    for k in range(1, rings):
        block = lax.rem(mc + k, rings)
        send(out_din.at[block], got_din.at[mc], (din_send.at[0], din_recv.at[0]), me, block).start()
    spread_value()
    got_din[mc] = out_din[mc]

    took(got_w, groups - 1, seq_recv.at[6])
    out_ws[...] = total(got_w)
    spread(7, out_ws, got_ws)
    got_ws[me] = out_ws[...]

    took(got_df, groups - 1, seq_recv.at[5])
    dfil_ref[...] = by_token(got_df[...]).astype(BF16)

    took(got_v, groups - 1, seq_recv.at[8])
    for part in range(2):
        half_sum = got_v[part].astype(F32)
        for p in range(part + 2, groups, 2):
            half_sum = half_sum + got_v[p].astype(F32)
        dw_ref[0, part * (ch_rows // 2):(part + 1) * (ch_rows // 2)] = half_sum.astype(BF16)
    took(got_din, rings - 1, din_recv.at[0])
    din_ref[...] = total(got_din)
    took(got_ws, groups - 1, seq_recv.at[7])
    size = parts * chans
    summed = got_ws[...].astype(F32)
    dw_ref[1] = by_width(summed[:, :size, :]).astype(BF16)
    dw_ref[2] = by_width(summed[:, size:, :]).astype(BF16)

    for array in range(2):
        block_to(array, mc, other, 0).wait_send()

        @pl.when(works)
        def _():
            for s in range(1, half):
                took(wholes[array], rings - 1, line_send.at[array, 1])

        @pl.when(rests)
        def _():
            block_to(array, mc, worker, 1).wait_send()

    @pl.when(works)
    def _():
        for stage, src in ((1, out_val), (2, out_dif)):
            took(src, half * groups - 1, seq_send.at[stage])
        for s in range(1, half):
            took(weights.at[s], splits - 1, share_send.at[s])

    @pl.when(rests)
    def _():
        share_up(slot).wait_send()

    pair_copy().wait_send()
    took(out_din, rings - 1, din_send.at[0])
    for stage, src in ((0, got_filt), (3, got_mix), (4, got_dv), (5, got_df), (6, got_w), (7, got_ws), (8, got_v)):
        took(src, groups - 1, seq_send.at[stage])


def finish(scale, din_ref, dw_ref, dfil_ref, din_out, dwv_out, dwg_out, dwo_out, dfil_out):
    din_out[...] = din_ref[...]
    dwv_out[...] = dw_ref[0].astype(F32) * scale
    dwg_out[...] = dw_ref[1].astype(F32) * scale
    dwo_out[...] = dw_ref[2].astype(F32) * scale
    dfil_out[...] = dfil_ref[...].astype(F32) * scale


def solution(mesh):
    groups, rings = mesh.shape["seq"], mesh.shape["ch"]

    def on_device(inputs, w_value, w_gate, w_out, filter_taps, grad_out):
        ch_rows, tokens = inputs.shape
        width = w_value.shape[0]
        chans, tiles, parts = ch_rows // groups, tokens // LANES, width // LANES
        tables = dft_tables(groups * tiles, LANES, chans)
        scale = 1.0 / math.sqrt(tokens * groups)
        vmem = pl.BlockSpec(memory_space=pltpu.VMEM)
        hbm = pl.BlockSpec(memory_space=pltpu.HBM)
        half = rings // 2
        flat = pltpu.VMEM((half * groups, tiles * chans, LANES), BF16)
        plane = pltpu.VMEM((groups, tiles * chans, LANES), BF16)
        whole = pltpu.VMEM((rings, ch_rows, tokens), BF16)
        splits = min(groups, ch_rows // 16)
        split = lambda w: w.reshape(splits, ch_rows // splits, width)
        share = pltpu.VMEM((groups, 2 * parts * chans, LANES), BF16)
        rows_of = pltpu.VMEM((ch_rows // 2, width), BF16)
        pair_of = pltpu.VMEM((2, ch_rows // 2, width), BF16)
        tokens_out = jax.ShapeDtypeStruct((ch_rows, tokens), F32)
        weight_out = jax.ShapeDtypeStruct((ch_rows, width), F32)
        d_inputs, d_weights, d_filter = pl.pallas_call(
            functools.partial(body, groups, rings),
            out_shape=(
                pltpu.VMEM((ch_rows, tokens), BF16),
                pltpu.VMEM((3, ch_rows, width), BF16),
                pltpu.VMEM((ch_rows, tokens), BF16),
            ),
            in_specs=[hbm] * 11,
            out_specs=(vmem,) * 3,
            scratch_shapes=[
                whole, whole, pltpu.VMEM((ch_rows, tokens), F32), pltpu.VMEM((half, splits, 3, ch_rows // splits, width), BF16),
                plane, plane, flat, plane, flat, plane] + [plane] * 6
            + [whole, whole]
            + [share, share, pltpu.VMEM((2 * parts * chans, LANES), BF16), share, pair_of, pltpu.VMEM((groups, ch_rows // 2, width), BF16), rows_of, rows_of]
            + [pltpu.VMEM((ch_rows, tokens), F32)] * 2
            + [pltpu.VMEM(table.shape, table.dtype) for table in tables] + [
                pltpu.SemaphoreType.DMA((12,)),
                pltpu.SemaphoreType.DMA((12,)),
                pltpu.SemaphoreType.DMA((1,)),
                pltpu.SemaphoreType.DMA((1,)),
                pltpu.SemaphoreType.DMA((2, 2)),
                pltpu.SemaphoreType.DMA((2, rings)),
                pltpu.SemaphoreType.DMA((half,)),
                pltpu.SemaphoreType.DMA((half, 2)),
                pltpu.SemaphoreType.DMA((5,)),
                pltpu.SemaphoreType.DMA((6,)),
                pltpu.SemaphoreType.REGULAR((len(near(groups)) + half - 2,)),
            ],
            compiler_params=pltpu.CompilerParams(collective_id=0, has_side_effects=True),
        )(
            inputs, split(w_value.T), split(w_gate.T), split(w_out), filter_taps, grad_out, *tables,
        )
        d_inputs, d_w_value, d_w_gate, d_w_out, d_filter = pl.pallas_call(
            functools.partial(finish, scale),
            out_shape=(
                jax.ShapeDtypeStruct((ch_rows, tokens), BF16), weight_out, weight_out, weight_out, tokens_out,
            ),
            in_specs=[vmem] * 3,
            out_specs=(vmem,) * 5,
            compiler_params=pltpu.CompilerParams(vmem_limit_bytes=8 << 20),
        )(d_inputs, d_weights, d_filter)
        return d_inputs, d_w_value.T, d_w_gate.T, d_w_out, d_filter

    return jax.shard_map(
        on_device,
        mesh=mesh,
        in_specs=(P("ch", "seq"), P(None, "ch"), P(None, "ch"), P("ch", None), P("ch", "seq"), P("ch", "seq")),
        out_specs=(P("ch", "seq"), P(None, "ch"), P(None, "ch"), P("ch", None), P("ch", "seq")),
        check_vma=False,
    )
```
